32 devices in a mesh: gx: 4 (over y, core), gy: 2 (over x), gz: 4 (over z).
Axes of the slice: x: 2, y: 2, z: 4, core: 2. Of those that a mesh axis runs over, the one named last changes fastest.
Arguments:
- thermal_state: float32 [32, 16, 512], P('gx', 'gy', 'gz'), may hold values from 0.5 to 1.5
- diffusivity: float32 [32, 16, 512], P('gx', 'gy', 'gz'), may hold values from 1.1 to 13.2
- staggered_flux_density: float32 [3, 32, 16, 512], P(None, 'gx', 'gy', 'gz'), may hold values from -6 to 6
- bulk_motion: float32 [3, 32, 16, 512], P(None, 'gx', 'gy', 'gz'), may hold values from -3 to 3
- mass_per_volume: float32 [32, 16, 512], P('gx', 'gy', 'gz'), may hold values from 0.5 to 2
Outputs:
- temperature_out: float32 [32, 16, 512], P('gx', 'gy', 'gz')
- face_field_out: float32 [3, 32, 16, 512], P(None, 'gx', 'gy', 'gz')
The draws below stay inside these ranges and needn't reach their ends.
All inputs are finite; a program needn't handle non-finite values.
Results may differ from the reference program's by a relative error of at most 0.00002.
Values sent between devices are 32-bit elements; how exact they have to be, the bound alone decides.
A program may use at most 128 MiB of HBM per device.

```python
import math
import jax
import jax.numpy as jnp
from jax import lax

SECTIONS = 8
EXTENT_LEADING = 32
EXTENT_MIDDLE = 16
EXTENT_TRAILING = 512


def draw_diffusivity(key, part):
    jitter_key = jax.random.fold_in(key, 11)
    jitter = jnp.exp(jax.random.uniform(jitter_key, (EXTENT_LEADING, EXTENT_MIDDLE, EXTENT_TRAILING), jnp.float32, math.log(0.5), math.log(2.0)))
    position = jnp.arange(EXTENT_LEADING, dtype=jnp.float32) / max(EXTENT_LEADING - 1, 1)
    growth = jnp.exp(math.log(3.0) * position)[:, None, None]
    return (2.2 * growth * jitter).astype(jnp.float32)


def block_levels(rng, extent, split, least, top_value):
    gain, own = 1.0, jax.random.fold_in(rng, 6)
    for axis_at, parts in split:
        draws = jnp.exp(jax.random.uniform(jax.random.fold_in(own, axis_at), (parts,), jnp.float32, least / len(split), top_value / len(split)))
        gain = gain * jnp.repeat(draws, extent[axis_at] // parts).reshape([-1 if axis == axis_at else 1 for axis in range(len(extent))])
    return gain


def bell_draw(rng, shape, scale, most, pieces=(), held_as=jnp.bfloat16):
    drawn = jax.random.normal(rng, shape, jnp.float32) * scale
    if len(pieces) > 0:
        drawn = block_levels(rng, shape, pieces, -0.22, 0.18) * drawn
    return jnp.clip(drawn, min=-most, max=most).astype(held_as)


def setup_inputs(seed: int = 0) -> dict:
    seeds = jax.random.split(jax.random.key(seed), 6)
    thermal_state = jnp.clip(0.5 + 1.0 * jax.random.uniform(seeds[0], (EXTENT_LEADING, EXTENT_MIDDLE, EXTENT_TRAILING), jnp.float32) ** block_levels(seeds[0], (EXTENT_LEADING, EXTENT_MIDDLE, EXTENT_TRAILING), ((0, 4), (1, 2), (2, 4)), -0.2, 0.2), 0.5, 1.5)
    diffusivity = draw_diffusivity(jax.random.fold_in(seeds[5], 71), 0)
    staggered_flux_density = bell_draw(seeds[2], (3, EXTENT_LEADING, EXTENT_MIDDLE, EXTENT_TRAILING), 1.0, 6.0, ((1, 4), (2, 2), (3, 4)), jnp.float32)
    bulk_motion = bell_draw(seeds[3], (3, EXTENT_LEADING, EXTENT_MIDDLE, EXTENT_TRAILING), 0.5, 3.0, ((1, 4), (2, 2), (3, 4)), jnp.float32)
    mass_per_volume = jnp.clip(jnp.exp(math.log(2.0) - 1.3862944 * jax.random.uniform(seeds[4], (EXTENT_LEADING, EXTENT_MIDDLE, EXTENT_TRAILING), jnp.float32) ** block_levels(seeds[4], (EXTENT_LEADING, EXTENT_MIDDLE, EXTENT_TRAILING), ((0, 4), (1, 2), (2, 4)), -0.2, 0.2)), 0.5, 2.0)
    return dict(thermal_state=thermal_state, diffusivity=diffusivity, staggered_flux_density=staggered_flux_density, bulk_motion=bulk_motion, mass_per_volume=mass_per_volume)


GAMMA = 5.0 / 3.0
FACE_FLOOR = 0.25
REFERENCE_SPOT = (0, 0, 0)

def unit_step(direction, amount):
    return tuple((amount if candidate == direction else 0 for candidate in range(3)))

def combine_steps(left_step, right_step):
    return tuple(map(lambda first_part, second_part: first_part + second_part, left_step, right_step))

def even_reach(amount):
    return (amount, amount, amount)

def sites_placed(source, ghost_layer_sites, offset, low_side, high_side):
    extents = source.shape[-3:]
    selector = [slice(None)] * (source.ndim - 3)
    for direction in range(3):
        interior = extents[direction] - 2 * ghost_layer_sites
        begin_at = ghost_layer_sites - low_side[direction] + offset[direction]
        selector.append(slice(begin_at, begin_at + interior + low_side[direction] + high_side[direction]))
    return source[tuple(selector)]

def trim_extent(source, ghost_layer_sites, amount):
    return sites_placed(source, ghost_layer_sites, REFERENCE_SPOT, even_reach(amount), even_reach(amount))

def face_coefficients(diffusion_coefficient, interface_quantities, ghost_layer_sites, reach):
    interior_block = even_reach(reach)
    lookup_arrays = []
    for normal in range(3):
        backward = unit_step(normal, -1)
        kappa_face = 0.5 * (sites_placed(diffusion_coefficient, ghost_layer_sites, REFERENCE_SPOT, interior_block, interior_block) + sites_placed(diffusion_coefficient, ghost_layer_sites, backward, interior_block, interior_block))
        normal_part = sites_placed(interface_quantities[normal], ghost_layer_sites, REFERENCE_SPOT, interior_block, interior_block)
        across = []
        for rotation in (1, 2):
            other_axis = (normal + rotation) % 3
            forward = unit_step(other_axis, 1)
            across.append(0.25 * (sites_placed(interface_quantities[other_axis], ghost_layer_sites, REFERENCE_SPOT, interior_block, interior_block) + sites_placed(interface_quantities[other_axis], ghost_layer_sites, forward, interior_block, interior_block) + sites_placed(interface_quantities[other_axis], ghost_layer_sites, backward, interior_block, interior_block) + sites_placed(interface_quantities[other_axis], ghost_layer_sites, combine_steps(backward, forward), interior_block, interior_block)))
        squared = normal_part * normal_part + across[0] * across[0] + across[1] * across[1]
        scaling = kappa_face / jnp.maximum(squared, FACE_FLOOR)
        lookup_arrays.append((scaling * normal_part * normal_part, scaling * normal_part * across[0], scaling * normal_part * across[1]))
    return lookup_arrays

def diffuse_thermal(profile, ghost_layer_sites, lookup_arrays, reach, target):
    interior_block = even_reach(target)
    balance = None
    for normal in range(3):
        upper_side = tuple((target + (1 if candidate == normal else 0) for candidate in range(3)))
        backward = unit_step(normal, -1)

        def shifted(offset):
            return sites_placed(profile, ghost_layer_sites, offset, interior_block, upper_side)
        slopes = []
        for rotation in (1, 2):
            other_axis = (normal + rotation) % 3
            forward = unit_step(other_axis, 1)
            rearward = unit_step(other_axis, -1)
            slopes.append(0.25 * (shifted(forward) - shifted(rearward) + shifted(combine_steps(backward, forward)) - shifted(combine_steps(backward, rearward))))
        along_normal, along_first, along_second = [sites_placed(coefficient, reach, REFERENCE_SPOT, interior_block, upper_side) for coefficient in lookup_arrays[normal]]
        face_flux = -(along_normal * (shifted(REFERENCE_SPOT) - shifted(backward)) + along_first * slopes[0] + along_second * slopes[1])
        length = face_flux.shape[normal]
        change = lax.slice_in_dim(face_flux, 1, length, axis=normal) - lax.slice_in_dim(face_flux, 0, length - 1, axis=normal)
        balance = -change if balance is None else balance - change
    return balance

def section_weights(total):
    first_rate = 4.0 / (total * total + total - 2)
    factors = [1.0 / 3.0, 1.0 / 3.0, 1.0 / 3.0]
    for ordinal in range(3, total + 1):
        factors.append((ordinal * ordinal + ordinal - 2) / (2.0 * ordinal * (ordinal + 1)))
    layout_recipe = [None, factors[1] * first_rate]
    for ordinal in range(2, total + 1):
        weight_prev = (2.0 * ordinal - 1.0) / ordinal * factors[ordinal] / factors[ordinal - 1]
        weight_older = -(ordinal - 1.0) / ordinal * factors[ordinal] / factors[ordinal - 2]
        rate_prev = weight_prev * first_rate
        rate_zero = -(1.0 - factors[ordinal - 1]) * rate_prev
        layout_recipe.append((weight_prev, weight_older, 1.0 - weight_prev - weight_older, rate_prev, rate_zero))
    return layout_recipe

def subdivision_advance(weights, interval_increment, newest_iterate, newest_extended, previous_iterate, previous_extended, initial, initial_margin, initial_derivative, zero_margin, lookup_arrays, reach):
    target = newest_extended - 1
    weight_prev, weight_older, weight_zero, rate_prev, rate_zero = weights
    prev_rate = diffuse_thermal(newest_iterate, newest_extended, lookup_arrays, reach, target)
    return weight_prev * trim_extent(newest_iterate, newest_extended, target) + weight_older * trim_extent(previous_iterate, previous_extended, target) + weight_zero * trim_extent(initial, initial_margin, target) + rate_prev * interval_increment * prev_rate + rate_zero * interval_increment * trim_extent(initial_derivative, zero_margin, target)

def fastest_characteristic(thermal_state, mass_per_volume, interface_quantities, bulk_motion, ghost_layer_sites):
    interior_block = even_reach(1)
    centred = []
    for direction in range(3):
        centred.append(0.5 * (sites_placed(interface_quantities[direction], ghost_layer_sites, REFERENCE_SPOT, interior_block, interior_block) + sites_placed(interface_quantities[direction], ghost_layer_sites, unit_step(direction, 1), interior_block, interior_block)))
    moving = [sites_placed(bulk_motion[direction], ghost_layer_sites, REFERENCE_SPOT, interior_block, interior_block) for direction in range(3)]
    field_square = centred[0] * centred[0] + centred[1] * centred[1] + centred[2] * centred[2]
    flow_speed = jnp.sqrt(moving[0] * moving[0] + moving[1] * moving[1] + moving[2] * moving[2])
    thermal_energy = sites_placed(thermal_state, ghost_layer_sites, REFERENCE_SPOT, interior_block, interior_block)
    inertia = sites_placed(mass_per_volume, ghost_layer_sites, REFERENCE_SPOT, interior_block, interior_block)
    return flow_speed + jnp.sqrt(GAMMA * thermal_energy + field_square / inertia)

def edge_fields(interface_quantities, face_margin, bulk_motion, ghost_layer_sites, propagation_rate):
    low_side = REFERENCE_SPOT
    high_side = (1, 1, 1)
    fields_out = []
    for edge_axis in range(3):
        first_axis = (edge_axis + 1) % 3
        second_axis = (edge_axis + 2) % 3
        back_first = unit_step(first_axis, -1)
        back_second = unit_step(second_axis, -1)
        back_both = combine_steps(back_first, back_second)

        def corner_mean(source, source_margin):
            return 0.25 * (sites_placed(source, source_margin, REFERENCE_SPOT, low_side, high_side) + sites_placed(source, source_margin, back_first, low_side, high_side) + sites_placed(source, source_margin, back_second, low_side, high_side) + sites_placed(source, source_margin, back_both, low_side, high_side))
        mean_first = corner_mean(bulk_motion[first_axis], ghost_layer_sites)
        mean_second = corner_mean(bulk_motion[second_axis], ghost_layer_sites)
        mean_speed = corner_mean(propagation_rate, 1)
        first_here = sites_placed(interface_quantities[first_axis], face_margin, REFERENCE_SPOT, low_side, high_side)
        first_below = sites_placed(interface_quantities[first_axis], face_margin, back_second, low_side, high_side)
        second_here = sites_placed(interface_quantities[second_axis], face_margin, REFERENCE_SPOT, low_side, high_side)
        second_below = sites_placed(interface_quantities[second_axis], face_margin, back_first, low_side, high_side)
        fields_out.append(mean_second * (0.5 * (first_here + first_below)) - mean_first * (0.5 * (second_here + second_below)) + 0.5 * mean_speed * (second_here - second_below) - 0.5 * mean_speed * (first_here - first_below))
    return fields_out

def edge_cells(source, offset):
    return source[tuple((slice(offset[candidate], offset[candidate] + source.shape[candidate] - 1) for candidate in range(3)))]

def faraday(interface_quantities, face_margin, edges, interval_increment):
    renewed_result = []
    for normal in range(3):
        next_axis = (normal + 1) % 3
        last_axis = (normal + 2) % 3
        curl_part = edge_cells(edges[last_axis], unit_step(next_axis, 1)) - edge_cells(edges[last_axis], REFERENCE_SPOT) - (edge_cells(edges[next_axis], unit_step(last_axis, 1)) - edge_cells(edges[next_axis], REFERENCE_SPOT))
        renewed_result.append(trim_extent(interface_quantities[normal], face_margin, 0) - interval_increment * curl_part)
    return jnp.stack(renewed_result)

def cyclic_wraparound(values, ghost_layer_sites):
    widths = [(0, 0)] * (values.ndim - 3) + [(ghost_layer_sites, ghost_layer_sites)] * 3
    return jnp.pad(values, widths, mode='wrap')

def reference(thermal_state, diffusivity, staggered_flux_density, bulk_motion, mass_per_volume):
    ghost_width = 2
    subdivision_width = 1
    thermal_state_extended = cyclic_wraparound(thermal_state, ghost_width)
    diffusivity_extended = cyclic_wraparound(diffusivity, ghost_width)
    staggered_extended = cyclic_wraparound(staggered_flux_density, ghost_width)
    velocity_extended = cyclic_wraparound(bulk_motion, ghost_width)
    mass_per_volume_extended = cyclic_wraparound(mass_per_volume, ghost_width)
    diffusion_coefficient = diffusivity_extended * jnp.power(thermal_state_extended, 2.5)
    limit_scale = (SECTIONS * SECTIONS + SECTIONS - 2) / 16.0
    interval_increment = jnp.min(limit_scale / trim_extent(diffusion_coefficient, ghost_width, 0))
    propagation_rate = fastest_characteristic(thermal_state_extended, mass_per_volume_extended, staggered_extended, velocity_extended, ghost_width)
    edges_now = edge_fields(staggered_extended, ghost_width, velocity_extended, ghost_width, propagation_rate)
    faces_mid = faraday(staggered_extended, ghost_width, edges_now, interval_increment)
    faces_mid_pad = cyclic_wraparound(faces_mid, 1)
    lookup_arrays = face_coefficients(diffusion_coefficient, staggered_extended, ghost_width, subdivision_width)
    initial_derivative = diffuse_thermal(thermal_state_extended, ghost_width, lookup_arrays, subdivision_width, subdivision_width - 1)
    layout_recipe = section_weights(SECTIONS)
    previous_iterate, previous_extended = (thermal_state_extended, ghost_width)
    newest_iterate = trim_extent(thermal_state_extended, ghost_width, subdivision_width - 1) + layout_recipe[1] * interval_increment * initial_derivative
    newest_extended = subdivision_width - 1
    for subdivision_number in range(2, SECTIONS + 1):
        if newest_extended == 0:
            newest_iterate = cyclic_wraparound(newest_iterate, subdivision_width)
            newest_extended = subdivision_width
        renewed_result = subdivision_advance(layout_recipe[subdivision_number], interval_increment, newest_iterate, newest_extended, previous_iterate, previous_extended, thermal_state_extended, ghost_width, initial_derivative, subdivision_width - 1, lookup_arrays, subdivision_width)
        previous_iterate, previous_extended = (newest_iterate, newest_extended)
        newest_iterate, newest_extended = (renewed_result, newest_extended - 1)
    edges_mid = edge_fields(faces_mid_pad, 1, velocity_extended, ghost_width, propagation_rate)
    faces_end = faraday(faces_mid_pad, 1, edges_mid, interval_increment)
    face_out = 0.5 * (trim_extent(staggered_extended, ghost_width, 0) + faces_end)
    return (newest_iterate, face_out)
```

```python
import functools
import operator

import jax
import jax.numpy as jnp
from jax import lax
from jax.experimental import pallas as pl
from jax.experimental.pallas import tpu as pltpu
from jax.sharding import PartitionSpec as P

SECTIONS = 8
GAMMA = 5.0 / 3.0
FACE_FLOOR = 0.25
MESH = pl.DeviceIdType.MESH
AXES = ("gx", "gy", "gz")
ROWS = 8
LANES = 128
WIDE = SECTIONS
THIN = 4
NWIDE = 5
NTHIN = 4


def section_weights(total):
    first_rate = 4.0 / (total * total + total - 2)
    factors = [1.0 / 3.0, 1.0 / 3.0, 1.0 / 3.0]
    for j in range(3, total + 1):
        factors.append((j * j + j - 2) / (2.0 * j * (j + 1)))
    recipe = [None, factors[1] * first_rate]
    for j in range(2, total + 1):
        p = (2.0 * j - 1.0) / j * factors[j] / factors[j - 1]
        r = -(j - 1.0) / j * factors[j] / factors[j - 2]
        m = p * first_rate
        h = -(1.0 - factors[j - 1]) * m
        recipe.append((p, r, 1.0 - p - r, m, h))
    return recipe


class Sheet:
    def __init__(self, parts):
        self.parts = parts

    def _with(self, other, op):
        if isinstance(other, Sheet):
            return Sheet([[op(a, b) for a, b in zip(p, q)] for p, q in zip(self.parts, other.parts)])
        return Sheet([[op(a, other) for a in p] for p in self.parts])

    def __add__(self, other):
        return self._with(other, operator.add)

    def __sub__(self, other):
        return self._with(other, operator.sub)

    def __mul__(self, other):
        return self._with(other, operator.mul)

    def __truediv__(self, other):
        return self._with(other, operator.truediv)

    def map(self, fn):
        return Sheet([[fn(a) for a in p] for p in self.parts])

    def y(self, step):
        n = len(self.parts)
        row = lax.broadcasted_iota(jnp.int32, (ROWS, LANES), 0)
        edge = row == (ROWS - 1 if step > 0 else 0)
        rolled = [[pltpu.roll(a, (-step) % ROWS, 0) for a in p] for p in self.parts]
        return Sheet(
            [
                [jnp.where(edge, b, a) for a, b in zip(rolled[c], rolled[(c + step) % n])]
                for c in range(n)
            ]
        )

    def z(self, step):
        lane = lax.broadcasted_iota(jnp.int32, (ROWS, LANES), 1)
        edge = lane == (LANES - 1 if step > 0 else 0)
        out = []
        for p in self.parts:
            a, b = [pltpu.roll(v, (-step) % LANES, 1) for v in p]
            out.append([jnp.where(edge, b, a), jnp.where(edge, a, b)])
        return Sheet(out)


def sqrt(sheet):
    return sheet.map(jnp.sqrt)


def get(ref, i):
    return Sheet([[ref[yc, zc, i] for zc in range(2)] for yc in range(ref.shape[0])])


def put(ref, i, sheet):
    for yc, p in enumerate(sheet.parts):
        for zc, v in enumerate(p):
            ref[yc, zc, i] = v


def flat(*sheets):
    return tuple(v for s in sheets for p in s.parts for v in p)


def unflat(values, nyc):
    size = 2 * nyc
    out = []
    for k in range(0, len(values), size):
        part = values[k : k + size]
        out.append(Sheet([list(part[2 * c : 2 * c + 2]) for c in range(nyc)]))
    return out


def centre(field):
    if field < NWIDE:
        return 2 * WIDE * field + WIDE
    return 2 * WIDE * NWIDE + 2 * THIN * (field - NWIDE) + THIN


def kernel(
    sizes, nx,
    t_in, d_in, b_in, v_in, r_in,
    t_out, b_out,
    fields, packed, mine, ends, kmax, parts_x, parts_y, parts_z,
    kappa, coef, ya, yb, rate0, speed, means, edges, mid,
    load_sem, red_send, red_recv, z_send, z_recv, y_send, y_recv, x_send, x_recv,
):
    counts = dict(zip(AXES, sizes))
    nyc = fields.shape[1]
    own = pl.ds(nx, nx)
    me = {a: lax.axis_index(a) for a in AXES}

    def at(axis, step):
        n = counts[axis]
        return {axis: lax.rem(me[axis] + (step % n), n)}

    def remote(src, dst, send, recv, device):
        return pltpu.make_async_remote_copy(
            src_ref=src, dst_ref=dst, send_sem=send, recv_sem=recv,
            device_id=device, device_id_type=MESH,
        )

    loads = [
        pltpu.make_async_copy(src, dst, load_sem.at[k])
        for k, (src, dst) in enumerate(
            (
                (t_in, fields.at[0, 0, 0, own]),
                (d_in, fields.at[1, 0, 0, own]),
                (b_in, fields.at[2:5, 0, 0, own]),
                (v_in, fields.at[5:8, 0, 0, own]),
                (r_in, fields.at[8, 0, 0, own]),
            )
        )
    ]
    for c in loads:
        c.start()
    barrier = pltpu.get_barrier_semaphore()
    greeted = 0
    for axis in AXES:
        for k in range(1, counts[axis]):
            pl.semaphore_signal(barrier, inc=1, device_id=at(axis, k), device_id_type=MESH)
            greeted += 1
    for c in loads:
        c.wait()

    lane = lax.broadcasted_iota(jnp.int32, (ROWS, LANES), 1)
    top = None
    for i in range(nx):
        t = fields[0, 0, 0, nx + i]
        k = fields[1, 0, 0, nx + i] * (t * t * jnp.sqrt(t))
        top = k if top is None else jnp.maximum(top, k)
    kmax[0] = top
    for i in range(nx):
        row = pltpu.roll(fields[0, 0, 0, nx + i], centre(0), 1)
        for f in range(1, NWIDE + NTHIN):
            start = centre(f) - (WIDE if f < NWIDE else THIN)
            row = jnp.where(lane >= start, pltpu.roll(fields[f, 0, 0, nx + i], centre(f), 1), row)
        mine[i] = row
    pl.semaphore_wait(barrier, greeted)

    sends = []

    def go(copies):
        for c in copies:
            c.start()
        sends.extend(copies)
        return copies

    slot = [0]

    def reduce_round(axis, src, dst):
        copies = []
        for k in range(1, counts[axis]):
            s = slot[0]
            slot[0] += 1
            copies.append(
                remote(src, dst.at[k - 1], red_send.at[s], red_recv.at[s], at(axis, k))
            )
        return copies

    def y_copies(s, ref):
        if nyc == 2:
            return [remote(ref(0), ref(1), y_send.at[s, 0], y_recv.at[s, 0], at("gy", 1))]
        return [
            remote(ref(0), ref(2), y_send.at[s, 0], y_recv.at[s, 0], at("gy", 1)),
            remote(ref(0), ref(1), y_send.at[s, 1], y_recv.at[s, 1], at("gy", -1)),
        ]

    def x_copies(s, ref, width):
        return [
            remote(
                ref(pl.ds(2 * nx - width, width)), ref(pl.ds(nx - width, width)),
                x_send.at[s, 0], x_recv.at[s, 0], at("gx", 1),
            ),
            remote(
                ref(pl.ds(nx, width)), ref(pl.ds(2 * nx, width)),
                x_send.at[s, 1], x_recv.at[s, 1], at("gx", -1),
            ),
        ]

    rest = pl.ds(1, nyc - 1)
    wide = pl.ds(0, NWIDE)
    thin = pl.ds(NWIDE, NTHIN)

    red_y = go(reduce_round("gy", kmax.at[0], parts_y))
    z_ends = go(
        [
            remote(mine, ends.at[0], z_send.at[0], z_recv.at[0], at("gz", 1)),
            remote(mine, ends.at[1], z_send.at[1], z_recv.at[1], at("gz", -1)),
        ]
    )
    y_wide = go(y_copies(0, lambda c: fields.at[wide, c, 0, own]))
    x_wide = go(x_copies(0, lambda r: fields.at[wide, 0, 0, r], nx))

    for c in red_y:
        c.wait_recv()
    for k in range(counts["gy"] - 1):
        top = jnp.maximum(top, parts_y[k])
    kmax[1] = top
    for c in z_ends:
        c.wait_recv()
    in_wide = lane < 2 * WIDE * NWIDE
    upper = jnp.where(in_wide, lane % (2 * WIDE) - WIDE, lane % (2 * THIN) - THIN) >= 0
    for i in range(nx):
        packed[0, nx + i] = jnp.where(upper, ends[1, i], ends[0, i])
    red_z = go(reduce_round("gz", kmax.at[1], parts_z))
    y_pack = go(y_copies(1, lambda c: packed.at[c, own]))
    y_thin = go(y_copies(2, lambda c: fields.at[thin, c, 0, own]))
    x_pack = go(x_copies(1, lambda r: packed.at[0, r], nx))

    for c in red_z:
        c.wait_recv()
    for k in range(counts["gz"] - 1):
        top = jnp.maximum(top, parts_z[k])
    kmax[2] = top
    for c in y_wide:
        c.wait_recv()
    red_x = go(reduce_round("gx", kmax.at[2], parts_x))
    x_wide2 = go(x_copies(2, lambda r: fields.at[wide, rest, 0, r], nx))
    for c in y_pack:
        c.wait_recv()
    x_pack2 = go(x_copies(3, lambda r: packed.at[rest, r], nx))
    x_thin = go(x_copies(4, lambda r: fields.at[thin, 0, 0, r], THIN))
    for c in y_thin:
        c.wait_recv()
    x_thin2 = go(x_copies(5, lambda r: fields.at[thin, rest, 0, r], THIN))
    for c in x_wide + x_pack + x_wide2 + x_pack2:
        c.wait_recv()

    def unpack(i, carry):
        for yc in range(nyc):
            pk = packed[yc, i]
            for f in range(NWIDE):
                fields[f, yc, 1, i] = pltpu.roll(pk, LANES - centre(f), 1)
            for zc in range(2):
                t = fields[0, yc, zc, i]
                kappa[yc, zc, i] = fields[1, yc, zc, i] * (t * t * jnp.sqrt(t))
        return carry

    lax.fori_loop(0, 3 * nx, unpack, 0)

    bx, by, bz = fields.at[2], fields.at[3], fields.at[4]
    t0 = fields.at[0]
    last = 3 * nx - 1

    def coefficients(i, carry):
        k0, km = get(kappa, i), get(kappa, i - 1)
        x0, xp = get(bx, i), get(bx, jnp.minimum(i + 1, last))
        y0, ym = get(by, i), get(by, i - 1)
        z0, zm = get(bz, i), get(bz, i - 1)

        def store(n, kf, bn, bo1, bo2):
            q = (bn * bn + bo1 * bo1 + bo2 * bo2).map(lambda v: jnp.maximum(v, FACE_FLOOR))
            s = kf / q * bn
            put(coef.at[3 * n], i, s * bn)
            put(coef.at[3 * n + 1], i, s * bo1 * 0.25)
            put(coef.at[3 * n + 2], i, s * bo2 * 0.25)

        sy, sz = y0 + ym, z0 + zm
        store(0, (k0 + km) * 0.5, x0, (sy + sy.y(1)) * 0.25, (sz + sz.z(1)) * 0.25)
        xx = x0 + xp
        zz = z0 + z0.z(1)
        store(1, (k0 + k0.y(-1)) * 0.5, y0, (zz + zz.y(-1)) * 0.25, (xx + xx.y(-1)) * 0.25)
        yy = y0 + y0.y(1)
        store(2, (k0 + k0.z(-1)) * 0.5, z0, (xx + xx.z(-1)) * 0.25, (yy + yy.z(-1)) * 0.25)
        return carry

    lax.fori_loop(1, 3 * nx, coefficients, 0)

    def conduct(u, reach, finish):
        def ahead(i, u0, u1, dy0, dz0):
            u1ym, u1zm = u1.y(-1), u1.z(-1)
            dy1, dz1 = u1.y(1) - u1ym, u1.z(1) - u1zm
            if u0 is None:
                return u1ym, u1zm, dy1, dz1, None
            gx = (
                get(coef.at[0], i) * (u1 - u0)
                + get(coef.at[1], i) * (dy1 + dy0)
                + get(coef.at[2], i) * (dz1 + dz0)
            )
            return u1ym, u1zm, dy1, dz1, gx

        first = nx - reach
        um, u0 = get(u, first - 1), get(u, first)
        _, _, dym, dzm, _ = ahead(first - 1, None, um, None, None)
        u0ym, u0zm, dy0, dz0, gx0 = ahead(first, um, u0, dym, dzm)

        def step(i, carry):
            um, u0, u0ym, u0zm, dy0, dz0, gx0 = unflat(carry, nyc)
            u1 = get(u, i + 1)
            u1ym, u1zm, dy1, dz1, gx1 = ahead(i + 1, u0, u1, dy0, dz0)
            dx = u1 - um
            gy = (
                get(coef.at[3], i) * (u0 - u0ym)
                + get(coef.at[4], i) * (dz0 + dz0.y(-1))
                + get(coef.at[5], i) * (dx + dx.y(-1))
            )
            gz = (
                get(coef.at[6], i) * (u0 - u0zm)
                + get(coef.at[7], i) * (dx + dx.z(-1))
                + get(coef.at[8], i) * (dy0 + dy0.z(-1))
            )
            finish(i, u0, (gx1 - gx0) + (gy.y(1) - gy) + (gz.z(1) - gz))
            return flat(u0, u1, u1ym, u1zm, dy1, dz1, gx1)

        lax.fori_loop(first, 2 * nx + reach, step, flat(um, u0, u0ym, u0zm, dy0, dz0, gx0))

    for c in red_x:
        c.wait_recv()
    for k in range(counts["gx"] - 1):
        top = jnp.maximum(top, parts_x[k])
    limit = (SECTIONS * SECTIONS + SECTIONS - 2) / 16.0
    peak = jnp.max(jnp.max(top, axis=0, keepdims=True), axis=1, keepdims=True)
    dt = jnp.broadcast_to(limit / peak, (ROWS, LANES))

    recipe = section_weights(SECTIONS)

    def begin(i, u0, rate):
        rate = rate * dt
        put(rate0, i, rate)
        put(ya, i, u0 + rate * recipe[1])

    conduct(t0, SECTIONS - 1, begin)
    newest, older = ya, yb
    for j in range(2, SECTIONS + 1):
        p, r, q, m, h = recipe[j]
        m_dt = dt * m
        prev2 = t0 if j == 2 else older

        def advance(i, u0, rate):
            value = (
                u0 * p + get(prev2, i) * r + get(t0, i) * q + rate * m_dt + get(rate0, i) * h
            )
            if j == SECTIONS:
                t_out[i - nx] = value.parts[0][0]
            else:
                put(older, i, value)

        conduct(newest, SECTIONS - j, advance)
        newest, older = older, newest

    for c in x_thin + x_thin2:
        c.wait_recv()
    vx, vy, vz = fields.at[5], fields.at[6], fields.at[7]
    rho = fields.at[8]

    def wave(i, carry):
        for yc in range(nyc):
            pk = packed[yc, i]
            for f in range(NWIDE, NWIDE + NTHIN):
                fields[f, yc, 1, i] = pltpu.roll(pk, LANES - centre(f), 1)
        y0, z0 = get(by, i), get(bz, i)
        cx = (get(bx, i) + get(bx, i + 1)) * 0.5
        cy = (y0 + y0.y(1)) * 0.5
        cz = (z0 + z0.z(1)) * 0.5
        a, b, c = get(vx, i), get(vy, i), get(vz, i)
        square = cx * cx + cy * cy + cz * cz
        put(
            speed, i,
            sqrt(a * a + b * b + c * c) + sqrt(get(t0, i) * GAMMA + square / get(rho, i)),
        )
        return carry

    lax.fori_loop(nx - 2, 2 * nx + 2, wave, 0)

    def corner_means(i, carry):
        s0, sm = get(speed, i), get(speed, i - 1)
        a, b, c = get(vx, i), get(vy, i), get(vz, i)
        am, bm, cm = get(vx, i - 1), get(vy, i - 1), get(vz, i - 1)

        def store(k, sheet, scale):
            put(means.at[k], i, sheet * scale)

        def along(s, direction):
            return s + (s.y(-1) if direction == 1 else s.z(-1))

        store(0, along(along(c, 1), 2), 0.125)
        store(1, along(along(b, 1), 2), 0.125)
        store(2, along(along(s0, 1), 2), 0.125)
        store(3, along(a + am, 2), 0.125)
        store(4, along(c + cm, 2), 0.125)
        store(5, along(s0 + sm, 2), 0.125)
        store(6, along(b + bm, 1), 0.125)
        store(7, along(a + am, 1), 0.125)
        store(8, along(s0 + sm, 1), 0.125)
        return carry

    lax.fori_loop(nx - 1, 2 * nx + 2, corner_means, 0)

    def edge_fields(fx, fy, fz, i):
        x0, y0, z0 = get(fx, i), get(fy, i), get(fz, i)
        ym, zm = get(fy, i - 1), get(fz, i - 1)

        def edge(k, a0, a1, b0, b1):
            mb, ma, ms = [get(means.at[3 * k + n], i) for n in range(3)]
            put(
                edges.at[k], i,
                mb * (a0 + a1) - ma * (b0 + b1) + ms * (b0 - b1) - ms * (a0 - a1),
            )

        edge(0, y0, y0.z(-1), z0, z0.y(-1))
        edge(1, z0, zm, x0, x0.z(-1))
        edge(2, x0, x0.y(-1), y0, ym)

    def curl(i):
        ex, ey, ez = [get(edges.at[n], i) for n in range(3)]
        eyp, ezp = get(edges.at[1], i + 1), get(edges.at[2], i + 1)
        return (
            (ez.y(1) - ez) - (ey.z(1) - ey),
            (ex.z(1) - ex) - (ezp - ez),
            (eyp - ey) - (ex.y(1) - ex),
        )

    def first_edges(i, carry):
        edge_fields(bx, by, bz, i)
        return carry

    lax.fori_loop(nx - 1, 2 * nx + 2, first_edges, 0)

    def to_mid(i, carry):
        for n, part in enumerate(curl(i)):
            put(mid.at[n], i, get(fields.at[2 + n], i) - part * dt)
        return carry

    lax.fori_loop(nx - 1, 2 * nx + 1, to_mid, 0)

    def second_edges(i, carry):
        edge_fields(mid.at[0], mid.at[1], mid.at[2], i)
        return carry

    lax.fori_loop(nx, 2 * nx + 1, second_edges, 0)

    def to_end(i, carry):
        for n, part in enumerate(curl(i)):
            end = get(mid.at[n], i) - part * dt
            value = (get(fields.at[2 + n], i) + end) * 0.5
            b_out[n, i - nx] = value.parts[0][0]
        return carry

    lax.fori_loop(nx, 2 * nx, to_end, 0)

    for c in sends:
        c.wait_send()


def solution(mesh):
    sizes = tuple(mesh.shape[a] for a in AXES)
    nyc = 2 if sizes[1] == 2 else 3

    def on_device(t, d, b, v, r):
        nx = t.shape[0]
        planes = 3 * nx
        tile = (ROWS, LANES)
        ring = (nyc, 2, planes) + tile
        vm = lambda *shape: pltpu.VMEM(shape, jnp.float32)
        rounds = sum(sizes) - 3
        return pl.pallas_call(
            functools.partial(kernel, sizes, nx),
            out_shape=(
                jax.ShapeDtypeStruct(t.shape, jnp.float32),
                jax.ShapeDtypeStruct(b.shape, jnp.float32),
            ),
            in_specs=[pl.BlockSpec(memory_space=pl.ANY)] * 5,
            out_specs=[pl.BlockSpec(memory_space=pltpu.VMEM)] * 2,
            scratch_shapes=[
                vm(NWIDE + NTHIN, *ring),
                vm(nyc, planes, *tile),
                vm(nx, *tile),
                vm(2, nx, *tile),
                vm(3, *tile),
                vm(sizes[0] - 1, *tile),
                vm(sizes[1] - 1, *tile),
                vm(sizes[2] - 1, *tile),
                vm(*ring),
                vm(9, *ring),
                vm(*ring),
                vm(*ring),
                vm(*ring),
                vm(*ring),
                vm(9, *ring),
                vm(3, *ring),
                vm(3, *ring),
                pltpu.SemaphoreType.DMA((5,)),
                pltpu.SemaphoreType.DMA((rounds,)),
                pltpu.SemaphoreType.DMA((rounds,)),
                pltpu.SemaphoreType.DMA((2,)),
                pltpu.SemaphoreType.DMA((2,)),
                pltpu.SemaphoreType.DMA((3, 2)),
                pltpu.SemaphoreType.DMA((3, 2)),
                pltpu.SemaphoreType.DMA((6, 2)),
                pltpu.SemaphoreType.DMA((6, 2)),
            ],
            compiler_params=pltpu.CompilerParams(
                collective_id=0, has_side_effects=True, vmem_limit_bytes=48 * 1024 * 1024
            ),
        )(t, d, b, v, r)

    return jax.shard_map(
        on_device,
        mesh=mesh,
        in_specs=(
            P("gx", "gy", "gz"),
            P("gx", "gy", "gz"),
            P(None, "gx", "gy", "gz"),
            P(None, "gx", "gy", "gz"),
            P("gx", "gy", "gz"),
        ),
        out_specs=(P("gx", "gy", "gz"), P(None, "gx", "gy", "gz")),
        check_vma=False,
    )
```

```python
import functools
import operator

import jax
import jax.numpy as jnp
from jax import lax
from jax.experimental import pallas as pl
from jax.experimental.pallas import tpu as pltpu
from jax.sharding import PartitionSpec as P

SECTIONS = 8
GAMMA = 5.0 / 3.0
FACE_FLOOR = 0.25
MESH = pl.DeviceIdType.MESH
AXES = ("gx", "gy", "gz")
ROWS = 8
LANES = 128
WIDE = SECTIONS
THIN = 4
NWIDE = 5
NTHIN = 4


def section_weights(total):
    first_rate = 4.0 / (total * total + total - 2)
    factors = [1.0 / 3.0, 1.0 / 3.0, 1.0 / 3.0]
    for j in range(3, total + 1):
        factors.append((j * j + j - 2) / (2.0 * j * (j + 1)))
    recipe = [None, factors[1] * first_rate]
    for j in range(2, total + 1):
        p = (2.0 * j - 1.0) / j * factors[j] / factors[j - 1]
        r = -(j - 1.0) / j * factors[j] / factors[j - 2]
        m = p * first_rate
        h = -(1.0 - factors[j - 1]) * m
        recipe.append((p, r, 1.0 - p - r, m, h))
    return recipe


class Sheet:
    def __init__(self, parts):
        self.parts = parts

    def _with(self, other, op):
        if isinstance(other, Sheet):
            return Sheet([[op(a, b) for a, b in zip(p, q)] for p, q in zip(self.parts, other.parts)])
        return Sheet([[op(a, other) for a in p] for p in self.parts])

    def __add__(self, other):
        return self._with(other, operator.add)

    def __sub__(self, other):
        return self._with(other, operator.sub)

    def __mul__(self, other):
        return self._with(other, operator.mul)

    def __truediv__(self, other):
        return self._with(other, operator.truediv)

    def map(self, fn):
        return Sheet([[fn(a) for a in p] for p in self.parts])

    def y(self, step):
        n = len(self.parts)
        row = lax.broadcasted_iota(jnp.int32, (ROWS, LANES), 0)
        edge = row == (ROWS - 1 if step > 0 else 0)
        rolled = [[pltpu.roll(a, (-step) % ROWS, 0) for a in p] for p in self.parts]
        return Sheet(
            [
                [jnp.where(edge, b, a) for a, b in zip(rolled[c], rolled[(c + step) % n])]
                for c in range(n)
            ]
        )

    def z(self, step):
        lane = lax.broadcasted_iota(jnp.int32, (ROWS, LANES), 1)
        edge = lane == (LANES - 1 if step > 0 else 0)
        out = []
        for p in self.parts:
            a, b = [pltpu.roll(v, (-step) % LANES, 1) for v in p]
            out.append([jnp.where(edge, b, a), jnp.where(edge, a, b)])
        return Sheet(out)


def sqrt(sheet):
    return sheet.map(jnp.sqrt)


def get(ref, i):
    return Sheet([[ref[yc, zc, i] for zc in range(2)] for yc in range(ref.shape[0])])


def put(ref, i, sheet):
    for yc, p in enumerate(sheet.parts):
        for zc, v in enumerate(p):
            ref[yc, zc, i] = v


def flat(*sheets):
    return tuple(v for s in sheets for p in s.parts for v in p)


def unflat(values, nyc):
    size = 2 * nyc
    out = []
    for k in range(0, len(values), size):
        part = values[k : k + size]
        out.append(Sheet([list(part[2 * c : 2 * c + 2]) for c in range(nyc)]))
    return out


def centre(field):
    if field < NWIDE:
        return 2 * WIDE * field + WIDE
    return 2 * WIDE * NWIDE + 2 * THIN * (field - NWIDE) + THIN


def kernel(
    sizes, nx,
    t_in, d_in, b_in, v_in, r_in,
    t_out, b_out,
    fields, packed, mine, ends, kmax, parts_x, parts_y, parts_z,
    kappa, coef, ya, yb, rate0, speed, means, edges, mid,
    load_sem, red_send, red_recv, z_send, z_recv, y_send, y_recv, x_send, x_recv,
):
    counts = dict(zip(AXES, sizes))
    nyc = fields.shape[1]
    own = pl.ds(nx, nx)
    me = {a: lax.axis_index(a) for a in AXES}

    def at(axis, step):
        n = counts[axis]
        return {axis: lax.rem(me[axis] + (step % n), n)}

    def remote(src, dst, send, recv, device):
        return pltpu.make_async_remote_copy(
            src_ref=src, dst_ref=dst, send_sem=send, recv_sem=recv,
            device_id=device, device_id_type=MESH,
        )

    loads = [
        pltpu.make_async_copy(src, dst, load_sem.at[k])
        for k, (src, dst) in enumerate(
            (
                (t_in, fields.at[0, 0, 0, own]),
                (d_in, fields.at[1, 0, 0, own]),
                (b_in, fields.at[2:5, 0, 0, own]),
                (v_in, fields.at[5:8, 0, 0, own]),
                (r_in, fields.at[8, 0, 0, own]),
            )
        )
    ]
    for c in loads:
        c.start()
    barrier = pltpu.get_barrier_semaphore()
    greeted = 0
    for axis in AXES:
        for k in range(1, counts[axis]):
            pl.semaphore_signal(barrier, inc=1, device_id=at(axis, k), device_id_type=MESH)
            greeted += 1
    for c in loads:
        c.wait()

    lane = lax.broadcasted_iota(jnp.int32, (ROWS, LANES), 1)
    top = None
    for i in range(nx):
        t = fields[0, 0, 0, nx + i]
        k = fields[1, 0, 0, nx + i] * (t * t * jnp.sqrt(t))
        top = k if top is None else jnp.maximum(top, k)
    kmax[0] = top
    for i in range(nx):
        row = pltpu.roll(fields[0, 0, 0, nx + i], centre(0), 1)
        for f in range(1, NWIDE + NTHIN):
            start = centre(f) - (WIDE if f < NWIDE else THIN)
            row = jnp.where(lane >= start, pltpu.roll(fields[f, 0, 0, nx + i], centre(f), 1), row)
        mine[i] = row
    pl.semaphore_wait(barrier, greeted)

    sends = []

    def go(copies):
        for c in copies:
            c.start()
        sends.extend(copies)
        return copies

    slot = [0]

    def reduce_round(axis, src, dst):
        copies = []
        for k in range(1, counts[axis]):
            s = slot[0]
            slot[0] += 1
            copies.append(
                remote(src, dst.at[k - 1], red_send.at[s], red_recv.at[s], at(axis, k))
            )
        return copies

    def y_copies(s, ref):
        if nyc == 2:
            return [remote(ref(0), ref(1), y_send.at[s, 0], y_recv.at[s, 0], at("gy", 1))]
        return [
            remote(ref(0), ref(2), y_send.at[s, 0], y_recv.at[s, 0], at("gy", 1)),
            remote(ref(0), ref(1), y_send.at[s, 1], y_recv.at[s, 1], at("gy", -1)),
        ]

    def x_copies(s, ref, width):
        return [
            remote(
                ref(pl.ds(2 * nx - width, width)), ref(pl.ds(nx - width, width)),
                x_send.at[s, 0], x_recv.at[s, 0], at("gx", 1),
            ),
            remote(
                ref(pl.ds(nx, width)), ref(pl.ds(2 * nx, width)),
                x_send.at[s, 1], x_recv.at[s, 1], at("gx", -1),
            ),
        ]

    rest = pl.ds(1, nyc - 1)
    wide = pl.ds(0, NWIDE)
    thin = pl.ds(NWIDE, NTHIN)

    red_y = go(reduce_round("gy", kmax.at[0], parts_y))
    z_ends = go(
        [
            remote(mine, ends.at[0], z_send.at[0], z_recv.at[0], at("gz", 1)),
            remote(mine, ends.at[1], z_send.at[1], z_recv.at[1], at("gz", -1)),
        ]
    )
    y_wide = go(y_copies(0, lambda c: fields.at[wide, c, 0, own]))
    x_wide = go(x_copies(0, lambda r: fields.at[wide, 0, 0, r], nx))

    for c in red_y:
        c.wait_recv()
    for k in range(counts["gy"] - 1):
        top = jnp.maximum(top, parts_y[k])
    kmax[1] = top
    for c in z_ends:
        c.wait_recv()
    in_wide = lane < 2 * WIDE * NWIDE
    upper = jnp.where(in_wide, lane % (2 * WIDE) - WIDE, lane % (2 * THIN) - THIN) >= 0
    for i in range(nx):
        packed[0, nx + i] = jnp.where(upper, ends[1, i], ends[0, i])
    red_z = go(reduce_round("gz", kmax.at[1], parts_z))
    y_pack = go(y_copies(1, lambda c: packed.at[c, own]))
    y_thin = go(y_copies(2, lambda c: fields.at[thin, c, 0, own]))
    x_pack = go(x_copies(1, lambda r: packed.at[0, r], nx))

    for c in red_z:
        c.wait_recv()
    for k in range(counts["gz"] - 1):
        top = jnp.maximum(top, parts_z[k])
    kmax[2] = top
    for c in y_wide:
        c.wait_recv()
    red_x = go(reduce_round("gx", kmax.at[2], parts_x))
    x_wide2 = go(x_copies(2, lambda r: fields.at[wide, rest, 0, r], nx))
    for c in y_pack:
        c.wait_recv()
    x_pack2 = go(x_copies(3, lambda r: packed.at[rest, r], nx))
    x_thin = go(x_copies(4, lambda r: fields.at[thin, 0, 0, r], THIN))
    for c in y_thin:
        c.wait_recv()
    x_thin2 = go(x_copies(5, lambda r: fields.at[thin, rest, 0, r], THIN))
    for c in x_wide + x_pack + x_wide2 + x_pack2:
        c.wait_recv()

    def unpack(i, carry):
        for yc in range(nyc):
            pk = packed[yc, i]
            for f in range(NWIDE):
                fields[f, yc, 1, i] = pltpu.roll(pk, LANES - centre(f), 1)
            for zc in range(2):
                t = fields[0, yc, zc, i]
                kappa[yc, zc, i] = fields[1, yc, zc, i] * (t * t * jnp.sqrt(t))
        return carry

    lax.fori_loop(0, 3 * nx, unpack, 0, unroll=3)

    bx, by, bz = fields.at[2], fields.at[3], fields.at[4]
    t0 = fields.at[0]
    last = 3 * nx - 1

    def coefficients(i, carry):
        k0, km = get(kappa, i), get(kappa, i - 1)
        x0, xp = get(bx, i), get(bx, jnp.minimum(i + 1, last))
        y0, ym = get(by, i), get(by, i - 1)
        z0, zm = get(bz, i), get(bz, i - 1)

        def store(n, kf, bn, bo1, bo2):
            q = (bn * bn + bo1 * bo1 + bo2 * bo2).map(lambda v: jnp.maximum(v, FACE_FLOOR))
            s = kf / q * bn
            put(coef.at[3 * n], i, s * bn)
            put(coef.at[3 * n + 1], i, s * bo1 * 0.25)
            put(coef.at[3 * n + 2], i, s * bo2 * 0.25)

        sy, sz = y0 + ym, z0 + zm
        store(0, (k0 + km) * 0.5, x0, (sy + sy.y(1)) * 0.25, (sz + sz.z(1)) * 0.25)
        xx = x0 + xp
        zz = z0 + z0.z(1)
        store(1, (k0 + k0.y(-1)) * 0.5, y0, (zz + zz.y(-1)) * 0.25, (xx + xx.y(-1)) * 0.25)
        yy = y0 + y0.y(1)
        store(2, (k0 + k0.z(-1)) * 0.5, z0, (xx + xx.z(-1)) * 0.25, (yy + yy.z(-1)) * 0.25)
        return carry

    lax.fori_loop(1, 3 * nx, coefficients, 0, unroll=2)

    def conduct(u, reach, finish):
        def ahead(i, u0, u1, dy0, dz0):
            u1ym, u1zm = u1.y(-1), u1.z(-1)
            dy1, dz1 = u1.y(1) - u1ym, u1.z(1) - u1zm
            if u0 is None:
                return u1ym, u1zm, dy1, dz1, None
            gx = (
                get(coef.at[0], i) * (u1 - u0)
                + get(coef.at[1], i) * (dy1 + dy0)
                + get(coef.at[2], i) * (dz1 + dz0)
            )
            return u1ym, u1zm, dy1, dz1, gx

        first = nx - reach
        um, u0 = get(u, first - 1), get(u, first)
        _, _, dym, dzm, _ = ahead(first - 1, None, um, None, None)
        u0ym, u0zm, dy0, dz0, gx0 = ahead(first, um, u0, dym, dzm)

        def step(i, carry):
            um, u0, u0ym, u0zm, dy0, dz0, gx0 = unflat(carry, nyc)
            u1 = get(u, i + 1)
            u1ym, u1zm, dy1, dz1, gx1 = ahead(i + 1, u0, u1, dy0, dz0)
            dx = u1 - um
            gy = (
                get(coef.at[3], i) * (u0 - u0ym)
                + get(coef.at[4], i) * (dz0 + dz0.y(-1))
                + get(coef.at[5], i) * (dx + dx.y(-1))
            )
            gz = (
                get(coef.at[6], i) * (u0 - u0zm)
                + get(coef.at[7], i) * (dx + dx.z(-1))
                + get(coef.at[8], i) * (dy0 + dy0.z(-1))
            )
            finish(i, u0, (gx1 - gx0) + (gy.y(1) - gy) + (gz.z(1) - gz))
            return flat(u0, u1, u1ym, u1zm, dy1, dz1, gx1)

        lax.fori_loop(first, 2 * nx + reach, step, flat(um, u0, u0ym, u0zm, dy0, dz0, gx0), unroll=4)

    for c in red_x:
        c.wait_recv()
    for k in range(counts["gx"] - 1):
        top = jnp.maximum(top, parts_x[k])
    limit = (SECTIONS * SECTIONS + SECTIONS - 2) / 16.0
    peak = jnp.max(jnp.max(top, axis=0, keepdims=True), axis=1, keepdims=True)
    dt = jnp.broadcast_to(limit / peak, (ROWS, LANES))

    recipe = section_weights(SECTIONS)

    def begin(i, u0, rate):
        rate = rate * dt
        put(rate0, i, rate)
        put(ya, i, u0 + rate * recipe[1])

    conduct(t0, SECTIONS - 1, begin)
    newest, older = ya, yb
    for j in range(2, SECTIONS + 1):
        p, r, q, m, h = recipe[j]
        m_dt = dt * m
        prev2 = t0 if j == 2 else older

        def advance(i, u0, rate):
            value = (
                u0 * p + get(prev2, i) * r + get(t0, i) * q + rate * m_dt + get(rate0, i) * h
            )
            if j == SECTIONS:
                t_out[i - nx] = value.parts[0][0]
            else:
                put(older, i, value)

        conduct(newest, SECTIONS - j, advance)
        newest, older = older, newest

    for c in x_thin + x_thin2:
        c.wait_recv()
    vx, vy, vz = fields.at[5], fields.at[6], fields.at[7]
    rho = fields.at[8]

    def wave(i, carry):
        for yc in range(nyc):
            pk = packed[yc, i]
            for f in range(NWIDE, NWIDE + NTHIN):
                fields[f, yc, 1, i] = pltpu.roll(pk, LANES - centre(f), 1)
        y0, z0 = get(by, i), get(bz, i)
        cx = (get(bx, i) + get(bx, i + 1)) * 0.5
        cy = (y0 + y0.y(1)) * 0.5
        cz = (z0 + z0.z(1)) * 0.5
        a, b, c = get(vx, i), get(vy, i), get(vz, i)
        square = cx * cx + cy * cy + cz * cz
        put(
            speed, i,
            sqrt(a * a + b * b + c * c) + sqrt(get(t0, i) * GAMMA + square / get(rho, i)),
        )
        return carry

    lax.fori_loop(nx - 2, 2 * nx + 2, wave, 0, unroll=4)

    def corner_means(i, carry):
        s0, sm = get(speed, i), get(speed, i - 1)
        a, b, c = get(vx, i), get(vy, i), get(vz, i)
        am, bm, cm = get(vx, i - 1), get(vy, i - 1), get(vz, i - 1)

        def store(k, sheet, scale):
            put(means.at[k], i, sheet * scale)

        def along(s, direction):
            return s + (s.y(-1) if direction == 1 else s.z(-1))

        store(0, along(along(c, 1), 2), 0.125)
        store(1, along(along(b, 1), 2), 0.125)
        store(2, along(along(s0, 1), 2), 0.125)
        store(3, along(a + am, 2), 0.125)
        store(4, along(c + cm, 2), 0.125)
        store(5, along(s0 + sm, 2), 0.125)
        store(6, along(b + bm, 1), 0.125)
        store(7, along(a + am, 1), 0.125)
        store(8, along(s0 + sm, 1), 0.125)
        return carry

    lax.fori_loop(nx - 1, 2 * nx + 2, corner_means, 0, unroll=4)

    def edge_fields(fx, fy, fz, i):
        x0, y0, z0 = get(fx, i), get(fy, i), get(fz, i)
        ym, zm = get(fy, i - 1), get(fz, i - 1)

        def edge(k, a0, a1, b0, b1):
            mb, ma, ms = [get(means.at[3 * k + n], i) for n in range(3)]
            put(
                edges.at[k], i,
                mb * (a0 + a1) - ma * (b0 + b1) + ms * (b0 - b1) - ms * (a0 - a1),
            )

        edge(0, y0, y0.z(-1), z0, z0.y(-1))
        edge(1, z0, zm, x0, x0.z(-1))
        edge(2, x0, x0.y(-1), y0, ym)

    def curl(i):
        ex, ey, ez = [get(edges.at[n], i) for n in range(3)]
        eyp, ezp = get(edges.at[1], i + 1), get(edges.at[2], i + 1)
        return (
            (ez.y(1) - ez) - (ey.z(1) - ey),
            (ex.z(1) - ex) - (ezp - ez),
            (eyp - ey) - (ex.y(1) - ex),
        )

    def first_edges(i, carry):
        edge_fields(bx, by, bz, i)
        return carry

    lax.fori_loop(nx - 1, 2 * nx + 2, first_edges, 0, unroll=4)

    def to_mid(i, carry):
        for n, part in enumerate(curl(i)):
            put(mid.at[n], i, get(fields.at[2 + n], i) - part * dt)
        return carry

    lax.fori_loop(nx - 1, 2 * nx + 1, to_mid, 0, unroll=4)

    def second_edges(i, carry):
        edge_fields(mid.at[0], mid.at[1], mid.at[2], i)
        return carry

    lax.fori_loop(nx, 2 * nx + 1, second_edges, 0, unroll=4)

    def to_end(i, carry):
        for n, part in enumerate(curl(i)):
            end = get(mid.at[n], i) - part * dt
            value = (get(fields.at[2 + n], i) + end) * 0.5
            b_out[n, i - nx] = value.parts[0][0]
        return carry

    lax.fori_loop(nx, 2 * nx, to_end, 0, unroll=4)

    for c in sends:
        c.wait_send()


def solution(mesh):
    sizes = tuple(mesh.shape[a] for a in AXES)
    nyc = 2 if sizes[1] == 2 else 3

    def on_device(t, d, b, v, r):
        nx = t.shape[0]
        planes = 3 * nx
        tile = (ROWS, LANES)
        ring = (nyc, 2, planes) + tile
        vm = lambda *shape: pltpu.VMEM(shape, jnp.float32)
        rounds = sum(sizes) - 3
        return pl.pallas_call(
            functools.partial(kernel, sizes, nx),
            out_shape=(
                jax.ShapeDtypeStruct(t.shape, jnp.float32),
                jax.ShapeDtypeStruct(b.shape, jnp.float32),
            ),
            in_specs=[pl.BlockSpec(memory_space=pltpu.HBM)] * 5,
            out_specs=[pl.BlockSpec(memory_space=pltpu.VMEM)] * 2,
            scratch_shapes=[
                vm(NWIDE + NTHIN, *ring),
                vm(nyc, planes, *tile),
                vm(nx, *tile),
                vm(2, nx, *tile),
                vm(3, *tile),
                vm(sizes[0] - 1, *tile),
                vm(sizes[1] - 1, *tile),
                vm(sizes[2] - 1, *tile),
                vm(*ring),
                vm(9, *ring),
                vm(*ring),
                vm(*ring),
                vm(*ring),
                vm(*ring),
                vm(9, *ring),
                vm(3, *ring),
                vm(3, *ring),
                pltpu.SemaphoreType.DMA((5,)),
                pltpu.SemaphoreType.DMA((rounds,)),
                pltpu.SemaphoreType.DMA((rounds,)),
                pltpu.SemaphoreType.DMA((2,)),
                pltpu.SemaphoreType.DMA((2,)),
                pltpu.SemaphoreType.DMA((3, 2)),
                pltpu.SemaphoreType.DMA((3, 2)),
                pltpu.SemaphoreType.DMA((6, 2)),
                pltpu.SemaphoreType.DMA((6, 2)),
            ],
            compiler_params=pltpu.CompilerParams(
                collective_id=0, has_side_effects=True, vmem_limit_bytes=67043328
            ),
        )(t, d, b, v, r)

    return jax.shard_map(
        on_device,
        mesh=mesh,
        in_specs=(
            P("gx", "gy", "gz"),
            P("gx", "gy", "gz"),
            P(None, "gx", "gy", "gz"),
            P(None, "gx", "gy", "gz"),
            P("gx", "gy", "gz"),
        ),
        out_specs=(P("gx", "gy", "gz"), P(None, "gx", "gy", "gz")),
        check_vma=False,
    )
```

```python
import functools
import operator

import jax
import jax.numpy as jnp
from jax import lax
from jax.experimental import pallas as pl
from jax.experimental.pallas import tpu as pltpu
from jax.sharding import PartitionSpec as P

SECTIONS = 8
GAMMA = 5.0 / 3.0
FACE_FLOOR = 0.25
MESH = pl.DeviceIdType.MESH
AXES = ("gx", "gy", "gz")
ROWS = 8
LANES = 128
WIDE = SECTIONS
THIN = 4
NEAR = 2
NWIDE = 5
NTHIN = 4


def section_weights(total):
    first_rate = 4.0 / (total * total + total - 2)
    factors = [1.0 / 3.0, 1.0 / 3.0, 1.0 / 3.0]
    for j in range(3, total + 1):
        factors.append((j * j + j - 2) / (2.0 * j * (j + 1)))
    recipe = [None, factors[1] * first_rate]
    for j in range(2, total + 1):
        p = (2.0 * j - 1.0) / j * factors[j] / factors[j - 1]
        r = -(j - 1.0) / j * factors[j] / factors[j - 2]
        m = p * first_rate
        h = -(1.0 - factors[j - 1]) * m
        recipe.append((p, r, 1.0 - p - r, m, h))
    return recipe


class Sheet:
    def __init__(self, parts):
        self.parts = parts

    def _with(self, other, op):
        if isinstance(other, Sheet):
            return Sheet([[op(a, b) for a, b in zip(p, q)] for p, q in zip(self.parts, other.parts)])
        return Sheet([[op(a, other) for a in p] for p in self.parts])

    def __add__(self, other):
        return self._with(other, operator.add)

    def __sub__(self, other):
        return self._with(other, operator.sub)

    def __mul__(self, other):
        return self._with(other, operator.mul)

    def __truediv__(self, other):
        return self._with(other, operator.truediv)

    def map(self, fn):
        return Sheet([[fn(a) for a in p] for p in self.parts])

    def y(self, step):
        n = len(self.parts)
        row = lax.broadcasted_iota(jnp.int32, (ROWS, LANES), 0)
        edge = row == (ROWS - 1 if step > 0 else 0)
        rolled = [[pltpu.roll(a, (-step) % ROWS, 0) for a in p] for p in self.parts]
        return Sheet(
            [
                [jnp.where(edge, b, a) for a, b in zip(rolled[c], rolled[(c + step) % n])]
                for c in range(n)
            ]
        )

    def z(self, step):
        lane = lax.broadcasted_iota(jnp.int32, (ROWS, LANES), 1)
        edge = lane == (LANES - 1 if step > 0 else 0)
        out = []
        for p in self.parts:
            a, b = [pltpu.roll(v, (-step) % LANES, 1) for v in p]
            out.append([jnp.where(edge, b, a), jnp.where(edge, a, b)])
        return Sheet(out)


def sqrt(sheet):
    return sheet.map(jnp.sqrt)


def get(ref, i):
    return Sheet([[ref[yc, zc, i] for zc in range(2)] for yc in range(ref.shape[0])])


def put(ref, i, sheet):
    for yc, p in enumerate(sheet.parts):
        for zc, v in enumerate(p):
            ref[yc, zc, i] = v


def flat(*sheets):
    return tuple(v for s in sheets for p in s.parts for v in p)


def unflat(values, nyc):
    size = 2 * nyc
    out = []
    for k in range(0, len(values), size):
        part = values[k : k + size]
        out.append(Sheet([list(part[2 * c : 2 * c + 2]) for c in range(nyc)]))
    return out


def centre(field):
    if field < NWIDE:
        return 2 * WIDE * field + WIDE
    return 2 * WIDE * NWIDE + 2 * THIN * (field - NWIDE) + THIN


def kernel(
    sizes, nx,
    t_in, d_in, b_in, v_in, r_in,
    t_out, b_out,
    fields, packed, mine, ends, kmax, parts_x, parts_y, parts_z,
    kappa, coef, ya, yb, rate0, speed, means, edges, mid,
    load_sem, red_send, red_recv, z_send, z_recv, y_send, y_recv, x_send, x_recv,
):
    counts = dict(zip(AXES, sizes))
    nyc = fields.shape[1]
    own = pl.ds(nx, nx)
    me = {a: lax.axis_index(a) for a in AXES}

    def at(axis, step):
        n = counts[axis]
        return {axis: lax.rem(me[axis] + (step % n), n)}

    def remote(src, dst, send, recv, device):
        return pltpu.make_async_remote_copy(
            src_ref=src, dst_ref=dst, send_sem=send, recv_sem=recv,
            device_id=device, device_id_type=MESH,
        )

    loads = [
        pltpu.make_async_copy(src, dst, load_sem.at[k])
        for k, (src, dst) in enumerate(
            (
                (t_in, fields.at[0, 0, 0, own]),
                (d_in, fields.at[1, 0, 0, own]),
                (b_in, fields.at[2:5, 0, 0, own]),
                (v_in, fields.at[5:8, 0, 0, own]),
                (r_in, fields.at[8, 0, 0, own]),
            )
        )
    ]
    for c in loads:
        c.start()
    barrier = pltpu.get_barrier_semaphore()
    greeted = 0
    for axis in AXES:
        for k in range(1, counts[axis]):
            pl.semaphore_signal(barrier, inc=1, device_id=at(axis, k), device_id_type=MESH)
            greeted += 1
    for c in loads:
        c.wait()

    lane = lax.broadcasted_iota(jnp.int32, (ROWS, LANES), 1)
    top = None
    for i in range(nx):
        t = fields[0, 0, 0, nx + i]
        k = fields[1, 0, 0, nx + i] * (t * t * jnp.sqrt(t))
        top = k if top is None else jnp.maximum(top, k)
    kmax[0] = top
    for i in range(nx):
        row = pltpu.roll(fields[0, 0, 0, nx + i], centre(0), 1)
        for f in range(1, NWIDE + NTHIN):
            start = centre(f) - (WIDE if f < NWIDE else THIN)
            row = jnp.where(lane >= start, pltpu.roll(fields[f, 0, 0, nx + i], centre(f), 1), row)
        mine[i] = row
    pl.semaphore_wait(barrier, greeted)

    sends = []

    def go(copies):
        for c in copies:
            c.start()
        sends.extend(copies)
        return copies

    slot = [0]

    def reduce_round(axis, src, dst):
        copies = []
        for k in range(1, counts[axis]):
            s = slot[0]
            slot[0] += 1
            copies.append(
                remote(src, dst.at[k - 1], red_send.at[s], red_recv.at[s], at(axis, k))
            )
        return copies

    def y_copies(s, ref):
        if nyc == 2:
            return [remote(ref(0), ref(1), y_send.at[s, 0], y_recv.at[s, 0], at("gy", 1))]
        return [
            remote(ref(0), ref(2), y_send.at[s, 0], y_recv.at[s, 0], at("gy", 1)),
            remote(ref(0), ref(1), y_send.at[s, 1], y_recv.at[s, 1], at("gy", -1)),
        ]

    def x_copies(s, ref, width):
        return [
            remote(
                ref(pl.ds(2 * nx - width, width)), ref(pl.ds(nx - width, width)),
                x_send.at[s, 0], x_recv.at[s, 0], at("gx", 1),
            ),
            remote(
                ref(pl.ds(nx, width)), ref(pl.ds(2 * nx, width)),
                x_send.at[s, 1], x_recv.at[s, 1], at("gx", -1),
            ),
        ]

    rest = pl.ds(1, nyc - 1)
    wide = pl.ds(0, NWIDE)
    thin = pl.ds(NWIDE, NTHIN)

    red_y = go(reduce_round("gy", kmax.at[0], parts_y))
    z_ends = go(
        [
            remote(mine, ends.at[0], z_send.at[0], z_recv.at[0], at("gz", 1)),
            remote(mine, ends.at[1], z_send.at[1], z_recv.at[1], at("gz", -1)),
        ]
    )
    pieces = (pl.ds(0, 2), pl.ds(2, 3))
    y_wide = [
        go(y_copies(n, lambda c, f=f: fields.at[f, c, 0, own])) for n, f in enumerate(pieces)
    ]
    x_wide = go(x_copies(0, lambda r: fields.at[wide, 0, 0, r], nx))

    for c in red_y:
        c.wait_recv()
    for k in range(counts["gy"] - 1):
        top = jnp.maximum(top, parts_y[k])
    kmax[1] = top
    red_z = go(reduce_round("gz", kmax.at[1], parts_z))
    for c in z_ends:
        c.wait_recv()
    in_wide = lane < 2 * WIDE * NWIDE
    upper = jnp.where(in_wide, lane % (2 * WIDE) - WIDE, lane % (2 * THIN) - THIN) >= 0
    for i in range(nx):
        packed[0, nx + i] = jnp.where(upper, ends[1, i], ends[0, i])
    for c in red_z:
        c.wait_recv()
    for k in range(counts["gz"] - 1):
        top = jnp.maximum(top, parts_z[k])
    kmax[2] = top
    y_pack = go(y_copies(2, lambda c: packed.at[c, own]))
    y_thin = go(y_copies(3, lambda c: fields.at[thin, c, 0, own]))
    x_pack = go(x_copies(1, lambda r: packed.at[0, r], nx))
    red_x = go(reduce_round("gx", kmax.at[2], parts_x))

    x_wide2 = []
    for n, f in enumerate(pieces):
        for c in y_wide[n]:
            c.wait_recv()
        x_wide2 += go(x_copies(2 + n, lambda r, f=f: fields.at[f, rest, 0, r], nx))
    for c in y_pack:
        c.wait_recv()
    x_pack2 = go(x_copies(4, lambda r: packed.at[rest, r], nx))
    x_thin = go(x_copies(5, lambda r: fields.at[thin, 0, 0, r], NEAR))

    def unpack(i, carry):
        for yc in range(nyc):
            pk = packed[yc, i]
            for f in range(NWIDE):
                fields[f, yc, 1, i] = pltpu.roll(pk, LANES - centre(f), 1)
            for zc in range(2):
                t = fields[0, yc, zc, i]
                kappa[yc, zc, i] = fields[1, yc, zc, i] * (t * t * jnp.sqrt(t))
        return carry

    lax.fori_loop(nx, 2 * nx, unpack, 0, unroll=4)

    bx, by, bz = fields.at[2], fields.at[3], fields.at[4]
    t0 = fields.at[0]
    last = 3 * nx - 1

    def coefficients(i, carry):
        k0, km = get(kappa, i), get(kappa, i - 1)
        x0, xp = get(bx, i), get(bx, jnp.minimum(i + 1, last))
        y0, ym = get(by, i), get(by, i - 1)
        z0, zm = get(bz, i), get(bz, i - 1)

        def store(n, kf, bn, bo1, bo2):
            q = (bn * bn + bo1 * bo1 + bo2 * bo2).map(lambda v: jnp.maximum(v, FACE_FLOOR))
            s = kf / q * bn
            put(coef.at[3 * n], i, s * bn)
            put(coef.at[3 * n + 1], i, s * bo1 * 0.25)
            put(coef.at[3 * n + 2], i, s * bo2 * 0.25)

        sy, sz = y0 + ym, z0 + zm
        store(0, (k0 + km) * 0.5, x0, (sy + sy.y(1)) * 0.25, (sz + sz.z(1)) * 0.25)
        xx = x0 + xp
        zz = z0 + z0.z(1)
        store(1, (k0 + k0.y(-1)) * 0.5, y0, (zz + zz.y(-1)) * 0.25, (xx + xx.y(-1)) * 0.25)
        yy = y0 + y0.y(1)
        store(2, (k0 + k0.z(-1)) * 0.5, z0, (xx + xx.z(-1)) * 0.25, (yy + yy.z(-1)) * 0.25)
        return carry

    lax.fori_loop(nx + 1, 2 * nx - 1, coefficients, 0, unroll=2)
    vx, vy, vz = fields.at[5], fields.at[6], fields.at[7]
    rho = fields.at[8]

    def wave(i, carry):
        for yc in range(nyc):
            pk = packed[yc, i]
            for f in range(NWIDE, NWIDE + NTHIN):
                fields[f, yc, 1, i] = pltpu.roll(pk, LANES - centre(f), 1)
        y0, z0 = get(by, i), get(bz, i)
        cx = (get(bx, i) + get(bx, i + 1)) * 0.5
        cy = (y0 + y0.y(1)) * 0.5
        cz = (z0 + z0.z(1)) * 0.5
        a, b, c = get(vx, i), get(vy, i), get(vz, i)
        square = cx * cx + cy * cy + cz * cz
        put(
            speed, i,
            sqrt(a * a + b * b + c * c) + sqrt(get(t0, i) * GAMMA + square / get(rho, i)),
        )
        return carry


    def corner_means(i, carry):
        s0, sm = get(speed, i), get(speed, i - 1)
        a, b, c = get(vx, i), get(vy, i), get(vz, i)
        am, bm, cm = get(vx, i - 1), get(vy, i - 1), get(vz, i - 1)

        def store(k, sheet, scale):
            put(means.at[k], i, sheet * scale)

        def along(s, direction):
            return s + (s.y(-1) if direction == 1 else s.z(-1))

        store(0, along(along(c, 1), 2), 0.125)
        store(1, along(along(b, 1), 2), 0.125)
        store(2, along(along(s0, 1), 2), 0.125)
        store(3, along(a + am, 2), 0.125)
        store(4, along(c + cm, 2), 0.125)
        store(5, along(s0 + sm, 2), 0.125)
        store(6, along(b + bm, 1), 0.125)
        store(7, along(a + am, 1), 0.125)
        store(8, along(s0 + sm, 1), 0.125)
        return carry


    def edge_fields(fx, fy, fz, i):
        x0, y0, z0 = get(fx, i), get(fy, i), get(fz, i)
        ym, zm = get(fy, i - 1), get(fz, i - 1)

        def edge(k, a0, a1, b0, b1):
            mb, ma, ms = [get(means.at[3 * k + n], i) for n in range(3)]
            put(
                edges.at[k], i,
                mb * (a0 + a1) - ma * (b0 + b1) + ms * (b0 - b1) - ms * (a0 - a1),
            )

        edge(0, y0, y0.z(-1), z0, z0.y(-1))
        edge(1, z0, zm, x0, x0.z(-1))
        edge(2, x0, x0.y(-1), y0, ym)

    def first_edges(i, carry):
        edge_fields(bx, by, bz, i)
        return carry

    for c in y_thin:
        c.wait_recv()
    x_thin2 = go(x_copies(6, lambda r: fields.at[thin, rest, 0, r], NEAR))
    lax.fori_loop(nx, 2 * nx - 1, wave, 0, unroll=2)
    lax.fori_loop(nx + 1, 2 * nx - 1, corner_means, 0, unroll=3)
    lax.fori_loop(nx + 1, 2 * nx - 1, first_edges, 0, unroll=3)

    for c in x_wide + x_pack + x_wide2 + x_pack2:
        c.wait_recv()
    lax.fori_loop(0, nx, unpack, 0, unroll=4)
    lax.fori_loop(2 * nx, 3 * nx, unpack, 0, unroll=4)
    lax.fori_loop(1, nx + 1, coefficients, 0, unroll=2)
    lax.fori_loop(2 * nx - 1, 3 * nx, coefficients, 0, unroll=3)


    def conduct(u, reach, finish):
        def ahead(i, u0, u1, dy0, dz0):
            u1ym, u1zm = u1.y(-1), u1.z(-1)
            dy1, dz1 = u1.y(1) - u1ym, u1.z(1) - u1zm
            if u0 is None:
                return u1ym, u1zm, dy1, dz1, None
            gx = (
                get(coef.at[0], i) * (u1 - u0)
                + get(coef.at[1], i) * (dy1 + dy0)
                + get(coef.at[2], i) * (dz1 + dz0)
            )
            return u1ym, u1zm, dy1, dz1, gx

        first = nx - reach
        um, u0 = get(u, first - 1), get(u, first)
        _, _, dym, dzm, _ = ahead(first - 1, None, um, None, None)
        u0ym, u0zm, dy0, dz0, gx0 = ahead(first, um, u0, dym, dzm)

        def step(i, carry):
            um, u0, u0ym, u0zm, dy0, dz0, gx0 = unflat(carry, nyc)
            u1 = get(u, i + 1)
            u1ym, u1zm, dy1, dz1, gx1 = ahead(i + 1, u0, u1, dy0, dz0)
            dx = u1 - um
            gy = (
                get(coef.at[3], i) * (u0 - u0ym)
                + get(coef.at[4], i) * (dz0 + dz0.y(-1))
                + get(coef.at[5], i) * (dx + dx.y(-1))
            )
            gz = (
                get(coef.at[6], i) * (u0 - u0zm)
                + get(coef.at[7], i) * (dx + dx.z(-1))
                + get(coef.at[8], i) * (dy0 + dy0.z(-1))
            )
            finish(i, u0, (gx1 - gx0) + (gy.y(1) - gy) + (gz.z(1) - gz))
            return flat(u0, u1, u1ym, u1zm, dy1, dz1, gx1)

        lax.fori_loop(first, 2 * nx + reach, step, flat(um, u0, u0ym, u0zm, dy0, dz0, gx0), unroll=4)

    for c in red_x:
        c.wait_recv()
    for k in range(counts["gx"] - 1):
        top = jnp.maximum(top, parts_x[k])
    limit = (SECTIONS * SECTIONS + SECTIONS - 2) / 16.0
    peak = jnp.max(jnp.max(top, axis=0, keepdims=True), axis=1, keepdims=True)
    dt = jnp.broadcast_to(limit / peak, (ROWS, LANES))

    recipe = section_weights(SECTIONS)

    def begin(i, u0, rate):
        rate = rate * dt
        put(rate0, i, rate)
        put(ya, i, u0 + rate * recipe[1])

    conduct(t0, SECTIONS - 1, begin)
    newest, older = ya, yb
    for j in range(2, SECTIONS + 1):
        p, r, q, m, h = recipe[j]
        m_dt = dt * m
        prev2 = t0 if j == 2 else older

        def advance(i, u0, rate):
            value = (
                u0 * p + get(prev2, i) * r + get(t0, i) * q + rate * m_dt + get(rate0, i) * h
            )
            if j == SECTIONS:
                t_out[i - nx] = value.parts[0][0]
            else:
                put(older, i, value)

        conduct(newest, SECTIONS - j, advance)
        newest, older = older, newest

    for c in x_thin + x_thin2:
        c.wait_recv()
    def curl(i):
        ex, ey, ez = [get(edges.at[n], i) for n in range(3)]
        eyp, ezp = get(edges.at[1], i + 1), get(edges.at[2], i + 1)
        return (
            (ez.y(1) - ez) - (ey.z(1) - ey),
            (ex.z(1) - ex) - (ezp - ez),
            (eyp - ey) - (ex.y(1) - ex),
        )

    for lo, hi in ((nx - 2, nx), (2 * nx - 1, 2 * nx + 2)):
        lax.fori_loop(lo, hi, wave, 0, unroll=hi - lo)
    for lo, hi in ((nx - 1, nx + 1), (2 * nx - 1, 2 * nx + 2)):
        lax.fori_loop(lo, hi, corner_means, 0, unroll=hi - lo)
        lax.fori_loop(lo, hi, first_edges, 0, unroll=hi - lo)

    def to_mid(i, carry):
        for n, part in enumerate(curl(i)):
            put(mid.at[n], i, get(fields.at[2 + n], i) - part * dt)
        return carry

    lax.fori_loop(nx - 1, 2 * nx + 1, to_mid, 0, unroll=4)

    def second_edges(i, carry):
        edge_fields(mid.at[0], mid.at[1], mid.at[2], i)
        return carry

    lax.fori_loop(nx, 2 * nx + 1, second_edges, 0, unroll=4)

    def to_end(i, carry):
        for n, part in enumerate(curl(i)):
            end = get(mid.at[n], i) - part * dt
            value = (get(fields.at[2 + n], i) + end) * 0.5
            b_out[n, i - nx] = value.parts[0][0]
        return carry

    lax.fori_loop(nx, 2 * nx, to_end, 0, unroll=4)

    for c in sends:
        c.wait_send()


def solution(mesh):
    sizes = tuple(mesh.shape[a] for a in AXES)
    nyc = 2 if sizes[1] == 2 else 3

    def on_device(t, d, b, v, r):
        nx = t.shape[0]
        planes = 3 * nx
        tile = (ROWS, LANES)
        ring = (nyc, 2, planes) + tile
        vm = lambda *shape: pltpu.VMEM(shape, jnp.float32)
        rounds = sum(sizes) - 3
        return pl.pallas_call(
            functools.partial(kernel, sizes, nx),
            out_shape=(
                jax.ShapeDtypeStruct(t.shape, jnp.float32),
                jax.ShapeDtypeStruct(b.shape, jnp.float32),
            ),
            in_specs=[pl.BlockSpec(memory_space=pltpu.HBM)] * 5,
            out_specs=[pl.BlockSpec(memory_space=pltpu.VMEM)] * 2,
            scratch_shapes=[
                vm(NWIDE + NTHIN, *ring),
                vm(nyc, planes, *tile),
                vm(nx, *tile),
                vm(2, nx, *tile),
                vm(3, *tile),
                vm(sizes[0] - 1, *tile),
                vm(sizes[1] - 1, *tile),
                vm(sizes[2] - 1, *tile),
                vm(*ring),
                vm(9, *ring),
                vm(*ring),
                vm(*ring),
                vm(*ring),
                vm(*ring),
                vm(9, *ring),
                vm(3, *ring),
                vm(3, *ring),
                pltpu.SemaphoreType.DMA((5,)),
                pltpu.SemaphoreType.DMA((rounds,)),
                pltpu.SemaphoreType.DMA((rounds,)),
                pltpu.SemaphoreType.DMA((2,)),
                pltpu.SemaphoreType.DMA((2,)),
                pltpu.SemaphoreType.DMA((4, 2)),
                pltpu.SemaphoreType.DMA((4, 2)),
                pltpu.SemaphoreType.DMA((7, 2)),
                pltpu.SemaphoreType.DMA((7, 2)),
            ],
            compiler_params=pltpu.CompilerParams(
                collective_id=0, has_side_effects=True, vmem_limit_bytes=67043328
            ),
        )(t, d, b, v, r)

    return jax.shard_map(
        on_device,
        mesh=mesh,
        in_specs=(
            P("gx", "gy", "gz"),
            P("gx", "gy", "gz"),
            P(None, "gx", "gy", "gz"),
            P(None, "gx", "gy", "gz"),
            P("gx", "gy", "gz"),
        ),
        out_specs=(P("gx", "gy", "gz"), P(None, "gx", "gy", "gz")),
        check_vma=False,
    )
```

```python
import functools
import operator

import jax
import jax.numpy as jnp
from jax import lax
from jax.experimental import pallas as pl
from jax.experimental.pallas import tpu as pltpu
from jax.sharding import PartitionSpec as P

SECTIONS = 8
GAMMA = 5.0 / 3.0
FACE_FLOOR = 0.25
MESH = pl.DeviceIdType.MESH
AXES = ("gx", "gy", "gz")
ROWS = 8
LANES = 128
WIDE = SECTIONS
THIN = 4
NEAR = 2
NWIDE = 5
NTHIN = 4


def section_weights(total):
    first_rate = 4.0 / (total * total + total - 2)
    factors = [1.0 / 3.0, 1.0 / 3.0, 1.0 / 3.0]
    for j in range(3, total + 1):
        factors.append((j * j + j - 2) / (2.0 * j * (j + 1)))
    recipe = [None, factors[1] * first_rate]
    for j in range(2, total + 1):
        p = (2.0 * j - 1.0) / j * factors[j] / factors[j - 1]
        r = -(j - 1.0) / j * factors[j] / factors[j - 2]
        m = p * first_rate
        h = -(1.0 - factors[j - 1]) * m
        recipe.append((p, r, 1.0 - p - r, m, h))
    return recipe


class Sheet:
    def __init__(self, parts):
        self.parts = parts

    def _with(self, other, op):
        if isinstance(other, Sheet):
            return Sheet([[op(a, b) for a, b in zip(p, q)] for p, q in zip(self.parts, other.parts)])
        return Sheet([[op(a, other) for a in p] for p in self.parts])

    def __add__(self, other):
        return self._with(other, operator.add)

    def __sub__(self, other):
        return self._with(other, operator.sub)

    def __mul__(self, other):
        return self._with(other, operator.mul)

    def __truediv__(self, other):
        return self._with(other, operator.truediv)

    def map(self, fn):
        return Sheet([[fn(a) for a in p] for p in self.parts])

    def y(self, step):
        n = len(self.parts)
        row = lax.broadcasted_iota(jnp.int32, (ROWS, LANES), 0)
        edge = row == (ROWS - 1 if step > 0 else 0)
        rolled = [[pltpu.roll(a, (-step) % ROWS, 0) for a in p] for p in self.parts]
        return Sheet(
            [
                [jnp.where(edge, b, a) for a, b in zip(rolled[c], rolled[(c + step) % n])]
                for c in range(n)
            ]
        )

    def z(self, step):
        lane = lax.broadcasted_iota(jnp.int32, (ROWS, LANES), 1)
        edge = lane == (LANES - 1 if step > 0 else 0)
        out = []
        for p in self.parts:
            a, b = [pltpu.roll(v, (-step) % LANES, 1) for v in p]
            out.append([jnp.where(edge, b, a), jnp.where(edge, a, b)])
        return Sheet(out)


def sqrt(sheet):
    return sheet.map(jnp.sqrt)


def get(ref, i):
    return Sheet([[ref[yc, zc, i] for zc in range(2)] for yc in range(ref.shape[0])])


def put(ref, i, sheet):
    for yc, p in enumerate(sheet.parts):
        for zc, v in enumerate(p):
            ref[yc, zc, i] = v


def flat(*sheets):
    return tuple(v for s in sheets for p in s.parts for v in p)


def unflat(values, nyc):
    size = 2 * nyc
    out = []
    for k in range(0, len(values), size):
        part = values[k : k + size]
        out.append(Sheet([list(part[2 * c : 2 * c + 2]) for c in range(nyc)]))
    return out


def centre(field):
    if field < NWIDE:
        return 2 * WIDE * field + WIDE
    return 2 * WIDE * NWIDE + 2 * THIN * (field - NWIDE) + THIN


def kernel(
    sizes, nx,
    t_in, d_in, b_in, v_in, r_in,
    t_out, b_out,
    fields, packed, mine, ends, kmax, parts_x, parts_y, parts_z,
    kappa, coef, ya, yb, rate0, speed, means, edges, mid,
    load_sem, red_send, red_recv, z_send, z_recv, y_send, y_recv, x_send, x_recv,
):
    counts = dict(zip(AXES, sizes))
    nyc = fields.shape[1]
    own = pl.ds(nx, nx)
    me = {a: lax.axis_index(a) for a in AXES}

    def at(axis, step):
        n = counts[axis]
        return {axis: lax.rem(me[axis] + (step % n), n)}

    def remote(src, dst, send, recv, device):
        return pltpu.make_async_remote_copy(
            src_ref=src, dst_ref=dst, send_sem=send, recv_sem=recv,
            device_id=device, device_id_type=MESH,
        )

    loads = [
        pltpu.make_async_copy(src, dst, load_sem.at[k])
        for k, (src, dst) in enumerate(
            (
                (t_in, fields.at[0, 0, 0, own]),
                (d_in, fields.at[1, 0, 0, own]),
                (b_in, fields.at[2:5, 0, 0, own]),
                (v_in, fields.at[5:8, 0, 0, own]),
                (r_in, fields.at[8, 0, 0, own]),
            )
        )
    ]
    for c in loads:
        c.start()
    barrier = pltpu.get_barrier_semaphore()
    greeted = 0
    for axis in AXES:
        for k in range(1, counts[axis]):
            pl.semaphore_signal(barrier, inc=1, device_id=at(axis, k), device_id_type=MESH)
            greeted += 1
    for c in loads:
        c.wait()

    lane = lax.broadcasted_iota(jnp.int32, (ROWS, LANES), 1)
    top = None
    for i in range(nx):
        t = fields[0, 0, 0, nx + i]
        k = fields[1, 0, 0, nx + i] * (t * t * jnp.sqrt(t))
        top = k if top is None else jnp.maximum(top, k)
    kmax[0] = top
    for i in range(nx):
        row = pltpu.roll(fields[0, 0, 0, nx + i], centre(0), 1)
        for f in range(1, NWIDE + NTHIN):
            start = centre(f) - (WIDE if f < NWIDE else THIN)
            row = jnp.where(lane >= start, pltpu.roll(fields[f, 0, 0, nx + i], centre(f), 1), row)
        mine[i] = row
    pl.semaphore_wait(barrier, greeted)

    sends = []

    def go(copies):
        for c in copies:
            c.start()
        sends.extend(copies)
        return copies

    slot = [0]

    def reduce_round(axis, src, dst):
        copies = []
        for k in range(1, counts[axis]):
            s = slot[0]
            slot[0] += 1
            copies.append(
                remote(src, dst.at[k - 1], red_send.at[s], red_recv.at[s], at(axis, k))
            )
        return copies

    def y_copies(s, ref):
        if nyc == 2:
            return [remote(ref(0), ref(1), y_send.at[s, 0], y_recv.at[s, 0], at("gy", 1))]
        return [
            remote(ref(0), ref(2), y_send.at[s, 0], y_recv.at[s, 0], at("gy", 1)),
            remote(ref(0), ref(1), y_send.at[s, 1], y_recv.at[s, 1], at("gy", -1)),
        ]

    def x_copies(s, ref, width):
        return [
            remote(
                ref(pl.ds(2 * nx - width, width)), ref(pl.ds(nx - width, width)),
                x_send.at[s, 0], x_recv.at[s, 0], at("gx", 1),
            ),
            remote(
                ref(pl.ds(nx, width)), ref(pl.ds(2 * nx, width)),
                x_send.at[s, 1], x_recv.at[s, 1], at("gx", -1),
            ),
        ]

    rest = pl.ds(1, nyc - 1)
    wide = pl.ds(0, NWIDE)
    thin = pl.ds(NWIDE, NTHIN)

    red_y = go(reduce_round("gy", kmax.at[0], parts_y))
    z_ends = go(
        [
            remote(mine, ends.at[0], z_send.at[0], z_recv.at[0], at("gz", 1)),
            remote(mine, ends.at[1], z_send.at[1], z_recv.at[1], at("gz", -1)),
        ]
    )
    pieces = (pl.ds(0, 2), pl.ds(2, 3))
    y_wide = [
        go(y_copies(n, lambda c, f=f: fields.at[f, c, 0, own])) for n, f in enumerate(pieces)
    ]
    x_wide = go(x_copies(0, lambda r: fields.at[wide, 0, 0, r], nx))

    for c in red_y:
        c.wait_recv()
    for k in range(counts["gy"] - 1):
        top = jnp.maximum(top, parts_y[k])
    kmax[1] = top
    red_z = go(reduce_round("gz", kmax.at[1], parts_z))
    for c in z_ends:
        c.wait_recv()
    in_wide = lane < 2 * WIDE * NWIDE
    upper = jnp.where(in_wide, lane % (2 * WIDE) - WIDE, lane % (2 * THIN) - THIN) >= 0
    for i in range(nx):
        packed[0, nx + i] = jnp.where(upper, ends[1, i], ends[0, i])
    for c in red_z:
        c.wait_recv()
    for k in range(counts["gz"] - 1):
        top = jnp.maximum(top, parts_z[k])
    kmax[2] = top
    y_pack = go(y_copies(2, lambda c: packed.at[c, own]))
    y_thin = go(y_copies(3, lambda c: fields.at[thin, c, 0, own]))
    x_pack = go(x_copies(1, lambda r: packed.at[0, r], nx))
    red_x = go(reduce_round("gx", kmax.at[2], parts_x))

    x_wide2 = []
    for n, f in enumerate(pieces):
        for c in y_wide[n]:
            c.wait_recv()
        x_wide2 += go(x_copies(2 + n, lambda r, f=f: fields.at[f, rest, 0, r], nx))
    for c in y_pack:
        c.wait_recv()
    x_pack2 = go(x_copies(4, lambda r: packed.at[rest, r], nx))
    x_thin = go(x_copies(5, lambda r: fields.at[thin, 0, 0, r], NEAR))

    def unpack(i, carry):
        for yc in range(nyc):
            pk = packed[yc, i]
            for f in range(NWIDE):
                fields[f, yc, 1, i] = pltpu.roll(pk, LANES - centre(f), 1)
            for zc in range(2):
                t = fields[0, yc, zc, i]
                kappa[yc, zc, i] = fields[1, yc, zc, i] * (t * t * jnp.sqrt(t))
        return carry

    lax.fori_loop(nx, 2 * nx, unpack, 0, unroll=4)

    bx, by, bz = fields.at[2], fields.at[3], fields.at[4]
    t0 = fields.at[0]
    last = 3 * nx - 1

    def coefficients(i, carry):
        k0, km = get(kappa, i), get(kappa, i - 1)
        x0, xp = get(bx, i), get(bx, jnp.minimum(i + 1, last))
        y0, ym = get(by, i), get(by, i - 1)
        z0, zm = get(bz, i), get(bz, i - 1)

        def store(n, kf, bn, bo1, bo2):
            q = (bn * bn + bo1 * bo1 + bo2 * bo2).map(lambda v: jnp.maximum(v, FACE_FLOOR))
            s = kf / q * bn
            put(coef.at[3 * n], i, s * bn)
            put(coef.at[3 * n + 1], i, s * bo1 * 0.25)
            put(coef.at[3 * n + 2], i, s * bo2 * 0.25)

        sy, sz = y0 + ym, z0 + zm
        store(0, (k0 + km) * 0.5, x0, (sy + sy.y(1)) * 0.25, (sz + sz.z(1)) * 0.25)
        xx = x0 + xp
        zz = z0 + z0.z(1)
        store(1, (k0 + k0.y(-1)) * 0.5, y0, (zz + zz.y(-1)) * 0.25, (xx + xx.y(-1)) * 0.25)
        yy = y0 + y0.y(1)
        store(2, (k0 + k0.z(-1)) * 0.5, z0, (xx + xx.z(-1)) * 0.25, (yy + yy.z(-1)) * 0.25)
        return carry

    lax.fori_loop(nx + 1, 2 * nx - 1, coefficients, 0, unroll=2)
    vx, vy, vz = fields.at[5], fields.at[6], fields.at[7]
    rho = fields.at[8]

    def wave(i, carry):
        for yc in range(nyc):
            pk = packed[yc, i]
            for f in range(NWIDE, NWIDE + NTHIN):
                fields[f, yc, 1, i] = pltpu.roll(pk, LANES - centre(f), 1)
        y0, z0 = get(by, i), get(bz, i)
        cx = (get(bx, i) + get(bx, i + 1)) * 0.5
        cy = (y0 + y0.y(1)) * 0.5
        cz = (z0 + z0.z(1)) * 0.5
        a, b, c = get(vx, i), get(vy, i), get(vz, i)
        square = cx * cx + cy * cy + cz * cz
        put(
            speed, i,
            sqrt(a * a + b * b + c * c) + sqrt(get(t0, i) * GAMMA + square / get(rho, i)),
        )
        return carry


    def corner_means(i, carry):
        s0, sm = get(speed, i), get(speed, i - 1)
        a, b, c = get(vx, i), get(vy, i), get(vz, i)
        am, bm, cm = get(vx, i - 1), get(vy, i - 1), get(vz, i - 1)

        def store(k, sheet, scale):
            put(means.at[k], i, sheet * scale)

        def along(s, direction):
            return s + (s.y(-1) if direction == 1 else s.z(-1))

        store(0, along(along(c, 1), 2), 0.125)
        store(1, along(along(b, 1), 2), 0.125)
        store(2, along(along(s0, 1), 2), 0.125)
        store(3, along(a + am, 2), 0.125)
        store(4, along(c + cm, 2), 0.125)
        store(5, along(s0 + sm, 2), 0.125)
        store(6, along(b + bm, 1), 0.125)
        store(7, along(a + am, 1), 0.125)
        store(8, along(s0 + sm, 1), 0.125)
        return carry


    def edge_fields(fx, fy, fz, i):
        x0, y0, z0 = get(fx, i), get(fy, i), get(fz, i)
        ym, zm = get(fy, i - 1), get(fz, i - 1)

        def edge(k, a0, a1, b0, b1):
            mb, ma, ms = [get(means.at[3 * k + n], i) for n in range(3)]
            put(
                edges.at[k], i,
                mb * (a0 + a1) - ma * (b0 + b1) + ms * (b0 - b1) - ms * (a0 - a1),
            )

        edge(0, y0, y0.z(-1), z0, z0.y(-1))
        edge(1, z0, zm, x0, x0.z(-1))
        edge(2, x0, x0.y(-1), y0, ym)

    def first_edges(i, carry):
        edge_fields(bx, by, bz, i)
        return carry

    for c in y_thin:
        c.wait_recv()
    x_thin2 = go(x_copies(6, lambda r: fields.at[thin, rest, 0, r], NEAR))
    lax.fori_loop(nx, 2 * nx - 1, wave, 0, unroll=2)
    lax.fori_loop(nx + 1, 2 * nx - 1, corner_means, 0, unroll=3)
    lax.fori_loop(nx + 1, 2 * nx - 1, first_edges, 0, unroll=3)

    for c in x_wide + x_pack + x_wide2 + x_pack2:
        c.wait_recv()
    lax.fori_loop(0, nx, unpack, 0, unroll=4)
    lax.fori_loop(2 * nx, 3 * nx, unpack, 0, unroll=4)
    lax.fori_loop(1, nx + 1, coefficients, 0, unroll=2)
    lax.fori_loop(2 * nx - 1, 3 * nx, coefficients, 0, unroll=3)


    def conduct(u, reach, finish):
        def ahead(i, u0, u1, dy0, dz0):
            u1ym, u1zm = u1.y(-1), u1.z(-1)
            dy1, dz1 = u1.y(1) - u1ym, u1.z(1) - u1zm
            if u0 is None:
                return u1ym, u1zm, dy1, dz1, None
            gx = (
                get(coef.at[0], i) * (u1 - u0)
                + get(coef.at[1], i) * (dy1 + dy0)
                + get(coef.at[2], i) * (dz1 + dz0)
            )
            return u1ym, u1zm, dy1, dz1, gx

        first = nx - reach
        um, u0 = get(u, first - 1), get(u, first)
        _, _, dym, dzm, _ = ahead(first - 1, None, um, None, None)
        u0ym, u0zm, dy0, dz0, gx0 = ahead(first, um, u0, dym, dzm)

        def step(i, carry):
            um, u0, u0ym, u0zm, dy0, dz0, gx0 = unflat(carry, nyc)
            u1 = get(u, i + 1)
            u1ym, u1zm, dy1, dz1, gx1 = ahead(i + 1, u0, u1, dy0, dz0)
            dx = u1 - um
            gy = (
                get(coef.at[3], i) * (u0 - u0ym)
                + get(coef.at[4], i) * (dz0 + dz0.y(-1))
                + get(coef.at[5], i) * (dx + dx.y(-1))
            )
            gz = (
                get(coef.at[6], i) * (u0 - u0zm)
                + get(coef.at[7], i) * (dx + dx.z(-1))
                + get(coef.at[8], i) * (dy0 + dy0.z(-1))
            )
            finish(i, u0, (gx1 - gx0) + (gy.y(1) - gy) + (gz.z(1) - gz))
            return flat(u0, u1, u1ym, u1zm, dy1, dz1, gx1)

        lax.fori_loop(first, 2 * nx + reach, step, flat(um, u0, u0ym, u0zm, dy0, dz0, gx0), unroll=(nx + 2 * reach) // 2)

    for c in red_x:
        c.wait_recv()
    for k in range(counts["gx"] - 1):
        top = jnp.maximum(top, parts_x[k])
    limit = (SECTIONS * SECTIONS + SECTIONS - 2) / 16.0
    peak = jnp.max(jnp.max(top, axis=0, keepdims=True), axis=1, keepdims=True)
    dt = jnp.broadcast_to(limit / peak, (ROWS, LANES))

    recipe = section_weights(SECTIONS)

    def begin(i, u0, rate):
        rate = rate * dt
        put(rate0, i, rate)
        put(ya, i, u0 + rate * recipe[1])

    conduct(t0, SECTIONS - 1, begin)
    newest, older = ya, yb
    for j in range(2, SECTIONS + 1):
        p, r, q, m, h = recipe[j]
        m_dt = dt * m
        prev2 = t0 if j == 2 else older

        def advance(i, u0, rate):
            value = (
                u0 * p + get(prev2, i) * r + get(t0, i) * q + rate * m_dt + get(rate0, i) * h
            )
            if j == SECTIONS:
                t_out[i - nx] = value.parts[0][0]
            else:
                put(older, i, value)

        conduct(newest, SECTIONS - j, advance)
        newest, older = older, newest

    for c in x_thin + x_thin2:
        c.wait_recv()
    def curl(i):
        ex, ey, ez = [get(edges.at[n], i) for n in range(3)]
        eyp, ezp = get(edges.at[1], i + 1), get(edges.at[2], i + 1)
        return (
            (ez.y(1) - ez) - (ey.z(1) - ey),
            (ex.z(1) - ex) - (ezp - ez),
            (eyp - ey) - (ex.y(1) - ex),
        )

    for lo, hi in ((nx - 2, nx), (2 * nx - 1, 2 * nx + 2)):
        lax.fori_loop(lo, hi, wave, 0, unroll=hi - lo)
    for lo, hi in ((nx - 1, nx + 1), (2 * nx - 1, 2 * nx + 2)):
        lax.fori_loop(lo, hi, corner_means, 0, unroll=hi - lo)
        lax.fori_loop(lo, hi, first_edges, 0, unroll=hi - lo)

    def to_mid(i, carry):
        for n, part in enumerate(curl(i)):
            put(mid.at[n], i, get(fields.at[2 + n], i) - part * dt)
        return carry

    lax.fori_loop(nx - 1, 2 * nx + 1, to_mid, 0, unroll=4)

    def second_edges(i, carry):
        edge_fields(mid.at[0], mid.at[1], mid.at[2], i)
        return carry

    lax.fori_loop(nx, 2 * nx + 1, second_edges, 0, unroll=4)

    def to_end(i, carry):
        for n, part in enumerate(curl(i)):
            end = get(mid.at[n], i) - part * dt
            value = (get(fields.at[2 + n], i) + end) * 0.5
            b_out[n, i - nx] = value.parts[0][0]
        return carry

    lax.fori_loop(nx, 2 * nx, to_end, 0, unroll=4)

    for c in sends:
        c.wait_send()


def solution(mesh):
    sizes = tuple(mesh.shape[a] for a in AXES)
    nyc = 2 if sizes[1] == 2 else 3

    def on_device(t, d, b, v, r):
        nx = t.shape[0]
        planes = 3 * nx
        tile = (ROWS, LANES)
        ring = (nyc, 2, planes) + tile
        vm = lambda *shape: pltpu.VMEM(shape, jnp.float32)
        rounds = sum(sizes) - 3
        return pl.pallas_call(
            functools.partial(kernel, sizes, nx),
            out_shape=(
                jax.ShapeDtypeStruct(t.shape, jnp.float32),
                jax.ShapeDtypeStruct(b.shape, jnp.float32),
            ),
            in_specs=[pl.BlockSpec(memory_space=pltpu.HBM)] * 5,
            out_specs=[pl.BlockSpec(memory_space=pltpu.VMEM)] * 2,
            scratch_shapes=[
                vm(NWIDE + NTHIN, *ring),
                vm(nyc, planes, *tile),
                vm(nx, *tile),
                vm(2, nx, *tile),
                vm(3, *tile),
                vm(sizes[0] - 1, *tile),
                vm(sizes[1] - 1, *tile),
                vm(sizes[2] - 1, *tile),
                vm(*ring),
                vm(9, *ring),
                vm(*ring),
                vm(*ring),
                vm(*ring),
                vm(*ring),
                vm(9, *ring),
                vm(3, *ring),
                vm(3, *ring),
                pltpu.SemaphoreType.DMA((5,)),
                pltpu.SemaphoreType.DMA((rounds,)),
                pltpu.SemaphoreType.DMA((rounds,)),
                pltpu.SemaphoreType.DMA((2,)),
                pltpu.SemaphoreType.DMA((2,)),
                pltpu.SemaphoreType.DMA((4, 2)),
                pltpu.SemaphoreType.DMA((4, 2)),
                pltpu.SemaphoreType.DMA((7, 2)),
                pltpu.SemaphoreType.DMA((7, 2)),
            ],
            compiler_params=pltpu.CompilerParams(
                collective_id=0, has_side_effects=True, vmem_limit_bytes=67043328
            ),
        )(t, d, b, v, r)

    return jax.shard_map(
        on_device,
        mesh=mesh,
        in_specs=(
            P("gx", "gy", "gz"),
            P("gx", "gy", "gz"),
            P(None, "gx", "gy", "gz"),
            P(None, "gx", "gy", "gz"),
            P("gx", "gy", "gz"),
        ),
        out_specs=(P("gx", "gy", "gz"), P(None, "gx", "gy", "gz")),
        check_vma=False,
    )
```
